256 devices in a mesh: rows: 64 (over z, y, core), sub: 4 (over x).
Axes of the slice: x: 4, y: 4, z: 8, core: 2. Of those that a mesh axis runs over, the one named last changes fastest.
Arguments:
- stiffness_tiles: bfloat16 [64, 4, 128, 128, 128], P('rows', 'sub'), may hold values from -0.5 to 0.5
- damping_tiles: bfloat16 [64, 4, 128, 128, 128], P('rows', 'sub'), may hold values from -0.5 to 0.5
- tile_map: int32 [64, 4, 2, 128], P('rows', 'sub'), may hold values from -1 to 767, as said below
- inv_mass: float32 [2097152], P(('rows', 'sub')), may hold values from 0.5 to 2
- spectral_shift: float32 [], replicated, may hold values from 0.5 to 1.5
- basis: float32 [58, 2097152], P(None, ('rows', 'sub')), may hold values from -20 to 20
- compact: float32 [2, 58, 57], replicated, may hold values from -0.54 to 0.54
Outputs:
- new_basis: float32 [2, 2097152], P(None, ('rows', 'sub'))
- compact_out: float32 [2, 60, 59], replicated
- hessenberg: float32 [59, 2], replicated
The draws below stay inside these ranges and needn't reach their ends.
Inputs may be any that keep to these rules, and one draw needn't show every extreme that they name: tile_map[r, s, 0, t] is the tile row of part r that slot t adds to, or -1 for an unused slot; the used slots of a device come first, and some device uses all 128. tile_map[r, s, 1, t] is the source column tile counted from the start of part r - 1.
All inputs are finite; a program needn't handle non-finite values.
Results may differ from the reference program's by a relative error of at most 0.0033.
Values may be sent and summed in bfloat16 or wider, within the bound.
A program may use at most 64 MiB of HBM per device.

```python
import math
import jax
import jax.numpy as jnp
from jax import lax

TILE = 128
RD = 8192
SLOTS = 128
K0 = 58
ITERS = 2
J0 = 57
NN = 2097152
N_ROWS = 64
N_SUB = 4


def draw_tile_map(key, part):
    tile_rows = N_SUB * RD // TILE
    device_count = N_ROWS * N_SUB
    keys = jax.random.split(key, 5)
    light = SLOTS // 8 + jax.random.randint(keys[0], (device_count,), 0, 3 * SLOTS // 8 + 1)
    chosen = jax.random.randint(keys[1], (device_count,), 0, 8) == 0
    forced = jax.random.randint(keys[2], (), 0, device_count)
    heavy = jnp.logical_or(chosen, jnp.arange(device_count) == forced)
    live_count = jnp.where(heavy, SLOTS, light)
    target = jax.random.randint(keys[3], (device_count, SLOTS), 0, tile_rows)
    offset = jax.random.randint(keys[4], (device_count, SLOTS), -tile_rows, tile_rows + 1)
    source = tile_rows + target + offset
    used_slots = jnp.arange(SLOTS)[None, :] < live_count[:, None]
    target = jnp.where(used_slots, target, -1)
    stacked = jnp.stack([target, source], axis=1)
    return stacked.reshape(N_ROWS, N_SUB, 2, SLOTS).astype(jnp.int32)


def draw_basis(key, part):
    unknowns = RD * N_ROWS * N_SUB
    keys = jax.random.split(key, 1)
    position = jnp.arange(unknowns, dtype=jnp.float32) / unknowns
    scaling = math.sqrt(math.log(3.0) / 4.0) * jnp.exp(math.log(3.0) * position)
    values = jax.random.normal(keys[0], (K0, unknowns), jnp.float32) * scaling[None, :]
    return jnp.clip(values, -20.0, 20.0)


def steps_of(own_key, shape, pieces, low, high):
    loudness = 1.0
    for axis_at, blocks in pieces:
        draws = jax.random.uniform(jax.random.fold_in(jax.random.fold_in(own_key, 6), axis_at), (blocks,), jnp.float32, low / len(pieces), high / len(pieces))
        loudness = loudness * jnp.repeat(jnp.exp(draws), shape[axis_at] // blocks).reshape((-1,) + (1,) * (len(shape) - 1 - axis_at))
    return loudness


def bell_draw(stream_key, extent, width, bound, cuts=(), held_as=jnp.bfloat16):
    entries = width * jax.random.normal(stream_key, extent, jnp.float32)
    if cuts:
        entries = entries * steps_of(stream_key, extent, cuts, -0.22, 0.18)
    return jnp.clip(entries, -bound, bound).astype(held_as)


def setup_inputs(seed: int = 0) -> dict:
    splits = jax.random.split(jax.random.key(seed), 8)
    stiffness_tiles = bell_draw(splits[0], (N_ROWS, N_SUB, SLOTS, TILE, TILE), (SLOTS * TILE * TILE // (2 * RD)) ** -0.5, 0.5, ((0, 64), (1, 4)))
    damping_tiles = bell_draw(splits[1], (N_ROWS, N_SUB, SLOTS, TILE, TILE), (SLOTS * TILE * TILE // (2 * RD)) ** -0.5, 0.5, ((0, 64), (1, 4)))
    tile_map = draw_tile_map(jax.random.fold_in(splits[7], 71), 0)
    inv_mass = jnp.clip(jnp.exp(math.log(2.0) - 1.3862944 * jax.random.uniform(splits[3], (NN,), jnp.float32) ** steps_of(splits[3], (NN,), ((0, 256),), -0.2, 0.2)), 0.5, 2.0)
    spectral_shift = jnp.clip(jax.random.uniform(splits[4], (), jnp.float32, 0.5, 1.5), 0.5, 1.5)
    basis = draw_basis(jax.random.fold_in(splits[7], 71), 0)
    compact = bell_draw(splits[6], (2, K0, J0), 0.09, 0.54, (), jnp.float32)
    return dict(stiffness_tiles=stiffness_tiles, damping_tiles=damping_tiles, tile_map=tile_map, inv_mass=inv_mass, spectral_shift=spectral_shift, basis=basis, compact=compact)


precise = lax.Precision.HIGHEST

def coupled_products(stiffness_tiles, damping_tiles, tile_map, vectors):
    part_rows = N_SUB * RD
    tile_rows = part_rows // TILE
    padded = jnp.pad(vectors, ((0, 0), (part_rows, part_rows)))
    blocked = padded.reshape(2, -1, TILE)

    def one_part(part_index):
        damping = damping_tiles[part_index].reshape(N_SUB * SLOTS, TILE, TILE).astype(jnp.float32)
        stiffness = stiffness_tiles[part_index].reshape(N_SUB * SLOTS, TILE, TILE).astype(jnp.float32)
        target = tile_map[part_index, :, 0, :].reshape(-1)
        source = tile_map[part_index, :, 1, :].reshape(-1)
        window = lax.dynamic_slice_in_dim(blocked, part_index * tile_rows, 3 * tile_rows, 1).astype(jnp.float32)
        picked = window[:, source]
        product = jnp.einsum('sij,sj->si', damping, picked[0], precision=precise)
        product = product + jnp.einsum('sij,sj->si', stiffness, picked[1], precision=precise)
        usable = target >= 0
        product = jnp.where(usable[:, None], product, jnp.zeros_like(product))
        summed = jax.ops.segment_sum(product, jnp.where(usable, target, 0), num_segments=tile_rows)
        return summed.reshape(-1)
    parts_out = lax.map(one_part, jnp.arange(N_ROWS, dtype=jnp.int32))
    return parts_out.reshape(-1)

def compact_update(upper_half, lower_half, coefficients, norm_value, lower_tail):
    columns = upper_half.shape[1]
    zero_row = jnp.zeros((1, columns), upper_half.dtype)
    upper_ext = jnp.concatenate([upper_half, zero_row], 0)
    lower_ext = jnp.concatenate([lower_half, zero_row], 0)
    upper_coeffs = jnp.concatenate([coefficients, norm_value[None]])
    lower_coeffs = jnp.concatenate([lower_tail, jnp.zeros((1,), lower_tail.dtype)])
    weights = jnp.zeros((columns,), upper_half.dtype)
    for repeat_index in range(2):
        projection = jnp.dot(upper_coeffs, upper_ext, precision=precise) + jnp.dot(lower_coeffs, lower_ext, precision=precise)
        upper_coeffs = upper_coeffs - jnp.dot(upper_ext, projection, precision=precise)
        lower_coeffs = lower_coeffs - jnp.dot(lower_ext, projection, precision=precise)
        weights = weights + projection
    beta_norm = jnp.sqrt(jnp.sum(upper_coeffs * upper_coeffs) + jnp.sum(lower_coeffs * lower_coeffs) + 1e-06)
    upper_new = jnp.concatenate([upper_ext, (upper_coeffs / beta_norm)[:, None]], 1)
    lower_new = jnp.concatenate([lower_ext, (lower_coeffs / beta_norm)[:, None]], 1)
    return (upper_new, lower_new, weights, beta_norm)

def reference(stiffness_tiles, damping_tiles, tile_map, inv_mass, spectral_shift, basis, compact):
    unknowns = RD * N_ROWS * N_SUB
    held = basis
    upper_half = compact[0]
    lower_half = compact[1]
    new_columns = []
    hess_columns = []
    for iteration in range(ITERS):
        upper_last = upper_half[:, -1]
        lower_last = lower_half[:, -1]
        upper_vec = jnp.dot(upper_last, held, precision=precise)
        lower_vec = jnp.dot(lower_last, held, precision=precise)
        vectors = jnp.stack([upper_vec, lower_vec]).astype(jnp.bfloat16)
        coupled = coupled_products(stiffness_tiles, damping_tiles, tile_map, vectors)
        image = spectral_shift * upper_vec - inv_mass * coupled
        first_part = jnp.dot(held, image, precision=precise) / unknowns
        residual_one = image - jnp.dot(first_part, held, precision=precise)
        second_part = jnp.dot(held, residual_one, precision=precise) / unknowns
        residual_two = residual_one - jnp.dot(second_part, held, precision=precise)
        coefficients = first_part + second_part
        norm_value = jnp.sqrt(jnp.sum(residual_two * residual_two) / unknowns + 1e-06)
        column = residual_two / norm_value
        lower_tail = upper_last + spectral_shift * lower_last
        upper_half, lower_half, weights, beta_norm = compact_update(upper_half, lower_half, coefficients, norm_value, lower_tail)
        held = jnp.concatenate([held, column[None]], 0)
        new_columns.append(column)
        hess_columns.append(jnp.concatenate([weights, beta_norm[None], jnp.zeros((ITERS - 1 - iteration,), weights.dtype)]))
    return (jnp.stack(new_columns), jnp.stack([upper_half, lower_half]), jnp.stack(hess_columns, axis=1))
```

```python
import functools

import jax
import jax.numpy as jnp
from jax import lax
from jax.experimental import pallas as pl
from jax.experimental.pallas import tpu as pltpu
from jax.sharding import PartitionSpec as P

ITERS = 2
EPS = 1e-06
GROUP = 16
MESH = pl.DeviceIdType.MESH
F32 = jnp.float32
BF16 = jnp.bfloat16


def dot_nt(a, b):
    return lax.dot_general(a, b, (((1,), (1,)), ((), ())), preferred_element_type=F32)


def halves(x):
    hi = x.astype(BF16)
    return hi, (x - hi.astype(F32)).astype(BF16)


def iota(shape, dim):
    return lax.broadcasted_iota(jnp.int32, shape, dim)


def lane_sum(x):
    return jnp.sum(x, axis=1, keepdims=True)


def row_sum(x):
    return jnp.sum(x, axis=0, keepdims=True)


class Plan:
    def __init__(self, rows, subs):
        self.rows, self.subs = rows, subs
        self.cores = 2
        self.ys = 4 if rows >= 32 else 2
        self.zs = rows // (self.ys * self.cores)
        self.plane = self.ys * subs
        self.line = self.zs * self.cores


def body(
    plan, k0, j0, unknowns, slots, tile_rows,
    stiff_hbm, damp_hbm, map_ref, mass_ref, shift_ref, basis_hbm, compact_ref,
    new_ref, comp_ref, hess_ref,
    tiles_d, tiles_k, nat, held, image_s, column_s, coef_u, coef_l, upper_m, lower_m, gram_m,
    split_s, onehot_g, onehot_s, window, part_s, part_r, parts_m, plane_r, line_r,
    gram_s, gram_1, gram_2, gram_3,
    tile_sem, basis_sem, send_sem, recv_sem,
):
    rows, subs = plan.rows, plan.subs
    row = lax.axis_index("rows")
    sub = lax.axis_index("sub")
    core = lax.rem(row, plan.cores)
    chip = lax.div(row, plan.cores)
    y = lax.rem(chip, plan.ys)
    z = lax.div(chip, plan.ys)
    in_plane = y * subs + sub
    in_line = z * plan.cores + core
    above = lax.rem(row + rows - 1, rows)
    below = lax.rem(row + 1, rows)

    def plane_peer(step):
        peer = lax.rem(in_plane + step, plan.plane)
        to_y, to_x = lax.div(peer, subs), lax.rem(peer, subs)
        return peer, ((z * plan.ys + to_y) * plan.cores + core, to_x)

    def line_peer(step):
        peer = lax.rem(in_line + step, plan.line)
        to_z, to_core = lax.div(peer, plan.cores), lax.rem(peer, plan.cores)
        return peer, ((to_z * plan.ys + y) * plan.cores + to_core, sub)

    barrier = pltpu.get_barrier_semaphore()

    def greet(device):
        pl.semaphore_signal(barrier, inc=1, device_id=device, device_id_type=MESH)

    def greet_plane(step, carry):
        greet(plane_peer(step)[1])
        return carry

    def greet_line(step, carry):
        greet(line_peer(step)[1])
        return carry

    def greet_beside(step, carry):
        greet((above, step))
        greet((below, step))
        return carry

    basis_copy = pltpu.make_async_copy(basis_hbm, nat, basis_sem)
    basis_copy.start()
    lax.fori_loop(0, subs, greet_beside, 0)
    lax.fori_loop(1, plan.plane, greet_plane, 0)
    lax.fori_loop(1, plan.line, greet_line, 0)
    copies = []
    for i, (hbm, ref) in enumerate(((damp_hbm, tiles_d), (stiff_hbm, tiles_k))):
        copy = pltpu.make_async_copy(hbm, ref, tile_sem.at[i])
        copy.start()
        copies.append(copy)

    def send(src, dst, which, device):
        pltpu.make_async_remote_copy(
            src_ref=src, dst_ref=dst, send_sem=send_sem.at[which], recv_sem=recv_sem.at[which],
            device_id=device, device_id_type=MESH,
        ).start()

    def arrived(view, which):
        pltpu.make_async_copy(view, view, recv_sem.at[which]).wait()

    def departed(view, which):
        pltpu.make_async_copy(view, view, send_sem.at[which]).wait()

    shift = shift_ref[0]
    scale = 1.0 / unknowns
    eye = (iota((128, 128), 0) == iota((128, 128), 1)).astype(F32)
    eye64 = (iota((64, 128), 0) == iota((64, 128), 1)).astype(F32)
    lane = iota((1, 128), 1)
    lane64 = iota((64, 128), 1)
    row64 = iota((64, 128), 0)

    upper_m[...] = jnp.zeros_like(upper_m)
    lower_m[...] = jnp.zeros_like(lower_m)
    upper_m[0:k0, 0:j0] = compact_ref[0]
    lower_m[0:k0, 0:j0] = compact_ref[1]
    u1 = lane_sum(jnp.where(lane64 == j0 - 1, upper_m[...], 0.0))
    u2 = lane_sum(jnp.where(lane64 == j0 - 1, lower_m[...], 0.0))
    u1 = jnp.broadcast_to(u1, (64, 128))
    u2 = jnp.broadcast_to(u2, (64, 128))
    coef_u[...] = u1
    coef_l[...] = u2
    column_s[...] = jnp.zeros_like(column_s)
    parts_m[...] = jnp.zeros_like(parts_m)
    split_s[...] = jnp.zeros_like(split_s)

    basis_copy.wait()
    nt = tile_rows

    def regroup(t, carry):
        held[pl.ds(t, k0, stride=nt), :] = nat[:, pl.ds(pl.multiple_of(t * 128, 128), 128)]
        return carry

    lax.fori_loop(0, nt, regroup, 0)

    def held_row(k):
        return held[pl.ds(pl.multiple_of(k * nt, 8), nt), :]

    def combined(refs):
        def add(k, totals):
            h = held_row(k)
            return tuple(
                total + h * jnp.broadcast_to(ref[pl.ds(k, 1), :], h.shape)
                for total, ref in zip(totals, refs)
            )
        return lax.fori_loop(0, k0, add, tuple(jnp.zeros((nt, 128), F32) for _ in refs))

    def exchange(it, upper, lower):
        mine = window.at[it, subs + sub]
        mine[...] = jnp.concatenate([upper, lower], axis=1).astype(BF16)
        which = it
        for step in range(1, subs):
            to = lax.rem(sub + step, subs)
            send(mine, window.at[it, subs + sub], which, (row, to))
        for step in range(subs):
            to = lax.rem(sub + step, subs)
            send(mine, window.at[it, sub], which, (below, to))
            send(mine, window.at[it, 2 * subs + sub], which, (above, to))

    upper, lower = combined((coef_u, coef_l))
    pl.semaphore_wait(barrier, plan.plane + plan.line - 2 + 2 * subs)
    exchange(0, upper, lower)

    wide = nat.shape[1] // 8

    def gram_part(c, total):
        piece = nat[:, pl.ds(pl.multiple_of(c * wide, 128), wide)]
        hi, lo = halves(piece)
        split_s[0:k0, :] = hi
        split_s[64 : 64 + k0, :] = lo
        return total + dot_nt(split_s[...], split_s[0:64, :])

    both = lax.fori_loop(0, 8, gram_part, jnp.zeros((128, 64), F32))
    cross = both[64:128]
    gram = both[0:64] + cross + cross.T
    gram = jnp.concatenate([gram, jnp.zeros((64, 64), F32)], axis=1)
    chunk = 64 // plan.plane
    for p in range(plan.plane):
        gram_s[p] = gram[p * chunk : (p + 1) * chunk]
    gram_1[in_plane] = gram_s[in_plane]

    def gram_out(step, carry):
        peer, device = plane_peer(step)
        send(gram_s.at[peer], gram_1.at[in_plane], 8, device)
        return carry

    lax.fori_loop(1, plan.plane, gram_out, 0)

    target = map_ref[0:1, :].astype(F32)
    source = map_ref[1:2, :].astype(F32)
    onehot_s[...] = (
        jnp.broadcast_to(target, onehot_s.shape) == iota(onehot_s.shape, 0).astype(F32)
    ).astype(F32).astype(BF16)
    eye_s = (iota((slots, slots), 0) == iota((slots, slots), 1)).astype(F32)
    source_col = lane_sum(jnp.broadcast_to(source, (slots, slots)) * eye_s)
    spot = iota(onehot_g.shape, 1)
    first_tile = jnp.where(row == 0, subs * nt, 0)
    last_tile = jnp.where(row == rows - 1, 2 * subs * nt, 3 * subs * nt)
    hit = (
        (jnp.broadcast_to(source_col, onehot_g.shape) == spot.astype(F32))
        & (spot >= first_tile) & (spot < last_tile)
    )
    onehot_g[...] = hit.astype(F32).astype(BF16)
    mass = mass_ref[...]
    block = min(16, slots)
    lane_s = iota((128, slots), 1)

    for it in range(ITERS):
        m, cols = k0 + it, j0 + it
        others = window.at[it, pl.ds(0, 3 * subs - 1)]
        arrived(others, it)
        departed(others, it)
        picked = jnp.dot(
            onehot_g[...], window[it].reshape(3 * subs * nt, 256), preferred_element_type=F32
        ).astype(BF16)
        if it == 0:
            for copy in copies:
                copy.wait()

        def products(b, total):
            d = tiles_d[pl.ds(b * block, block)].reshape(block * 128, 128)
            k = tiles_k[pl.ds(b * block, block)].reshape(block * 128, 128)
            r = dot_nt(jnp.concatenate([d, k], axis=1), picked)
            for i in range(block):
                total = jnp.where(lane_s == b * block + i, r[i * 128 : (i + 1) * 128], total)
            return total

        product = lax.fori_loop(0, slots // block, products, jnp.zeros((128, slots), F32))
        hi, lo = halves(product)
        part = dot_nt(onehot_s[...], hi) + dot_nt(onehot_s[...], lo)
        part_s[it] = part.reshape(subs, nt, 128)
        for step in range(1, subs):
            to = lax.rem(sub + step, subs)
            send(part_s.at[it, to], part_r.at[it, step - 1], 2 + it, (row, to))
        if it == 0:
            rest = gram_1.at[pl.ds(0, plan.plane - 1)]
            arrived(rest, 8)
            departed(rest, 8)
            gram_2[in_line] = jnp.sum(gram_1[...], axis=0)

            def gram_on(step, carry):
                send(gram_2.at[in_line], gram_2.at[in_line], 9, line_peer(step)[1])
                return carry

            lax.fori_loop(1, plan.line, gram_on, 0)
        own = part_s[it, sub]
        arrived(part_r.at[it], 2 + it)
        departed(part_r.at[it], 2 + it)
        coupled = own + part_r[it, 0]
        for step in range(2, subs):
            coupled = coupled + part_r[it, step - 1]
        image = shift * upper - mass * coupled
        image_s[...] = image
        if it == 0:
            rest = gram_2.at[pl.ds(0, plan.line - 1)]
            arrived(rest, 9)
            departed(rest, 9)
            gram_3[in_plane] = jnp.sum(gram_2[...], axis=0)

            def gram_back(step, carry):
                send(gram_3.at[in_plane], gram_3.at[in_plane], 10, plane_peer(step)[1])
                return carry

            lax.fori_loop(1, plan.plane, gram_back, 0)

        def inner(t, total):
            piece = nat[:, pl.ds(pl.multiple_of(t * 128, 128), 128)]
            return total + piece * jnp.broadcast_to(image_s[pl.ds(t, 1), :], piece.shape)

        parts_m[0:k0, :] = lax.fori_loop(0, nt, inner, jnp.zeros((k0, 128), F32))
        if it > 0:
            parts_m[k0 : k0 + 1, :] = row_sum(column_s[...] * image)
        parts_m[63:64, :] = row_sum(image * image)
        line = row_sum(parts_m[...].T)
        plane_r[it, in_plane] = line

        def plane_out(step, carry):
            spot = plane_r.at[it, in_plane]
            send(spot, spot, 4 + it, plane_peer(step)[1])
            return carry

        lax.fori_loop(1, plan.plane, plane_out, 0)
        if it == 0:
            rest = gram_3.at[pl.ds(0, plan.plane - 1)]
            arrived(rest, 10)
            departed(rest, 10)
            gram_m[...] = gram_3[...].reshape(64, 128) * scale
        rest = plane_r.at[it, pl.ds(0, plan.plane - 1)]
        arrived(rest, 4 + it)
        departed(rest, 4 + it)
        line_r[it, in_line] = jnp.sum(plane_r[it], axis=0)

        def line_out(step, carry):
            spot = line_r.at[it, in_line]
            send(spot, spot, 6 + it, line_peer(step)[1])
            return carry

        lax.fori_loop(1, plan.line, line_out, 0)
        gram = gram_m[...]
        rest = line_r.at[it, pl.ds(0, plan.line - 1)]
        arrived(rest, 6 + it)
        departed(rest, 6 + it)
        sums = jnp.sum(line_r[it], axis=0) * scale

        own_square = lane_sum(jnp.where(lane == 63, sums, 0.0))
        first = jnp.where(lane < m, sums, 0.0)
        coef = lane_sum((2.0 * eye64 - gram) * first)
        coef = jnp.broadcast_to(coef, (64, 128))
        coef_row = row_sum(eye64 * coef)
        gram_coef = row_sum(gram * coef)
        square = own_square + lane_sum(coef_row * (gram_coef - 2.0 * first))
        norm = jnp.sqrt(square + EPS)

        up, low = upper_m[...], lower_m[...]
        upper_c = jnp.where(row64 == m, norm, coef)
        lower_c = u1 + shift * u2
        weights = jnp.zeros((1, 128), F32)
        for _ in range(2):
            projection = row_sum(up * upper_c + low * lower_c)
            upper_c = upper_c - lane_sum(up * projection)
            lower_c = lower_c - lane_sum(low * projection)
            weights = weights + projection
        beta = jnp.sqrt(
            row_sum(upper_c * upper_c) + row_sum(lower_c * lower_c) + EPS
        )
        u1, u2 = upper_c / beta, lower_c / beta
        weights = jnp.where(lane == cols, beta, weights)
        hess = lane_sum(eye64 * weights)
        hess_ref[:, it : it + 1] = hess[0 : j0 + ITERS]

        if it + 1 < ITERS:
            tail = row_sum(jnp.where(row64 == m, u1, 0.0))
            ratio = tail / norm
            coef_u[...] = u1 - ratio * coef
            coef_l[...] = u2
            held_u, lower = combined((coef_u, coef_l))
            upper = held_u + ratio * image
            exchange(it + 1, upper, lower)
        up = jnp.where(lane64 == cols, u1, up)
        low = jnp.where(lane64 == cols, u2, low)
        upper_m[...] = up
        lower_m[...] = low
        coef_u[...] = coef
        (taken,) = combined((coef_u,))
        if it > 0:
            taken = taken + row_sum(jnp.where(row64 == k0, coef, 0.0)) * column_s[...]
        column_s[...] = (image - taken) / norm
        for t in range(nt):
            new_ref[it : it + 1, t * 128 : (t + 1) * 128] = column_s[t : t + 1, :]
        if it + 1 < ITERS:
            cross_row = (first - gram_coef) / norm
            cross_col = lane_sum(eye64 * cross_row)
            gram = jnp.where(row64 == m, cross_row, gram)
            gram = jnp.where(lane64 == m, cross_col, gram)
            gram = jnp.where((row64 == m) & (lane64 == m), square / (norm * norm), gram)
            gram_m[...] = gram
    comp_ref[0] = upper_m[0 : k0 + ITERS, 0 : j0 + ITERS]
    comp_ref[1] = lower_m[0 : k0 + ITERS, 0 : j0 + ITERS]


def on_device(stiffness, damping, tile_map, mass, shift, basis, compact, *, rows, subs):
    plan = Plan(rows, subs)
    k0, local = basis.shape
    j0 = compact.shape[2]
    slots = stiffness.shape[2]
    nt = local // 128
    unknowns = local * rows * subs
    chunk = 64 // plan.plane
    vmem = pl.BlockSpec(memory_space=pltpu.VMEM)
    hbm = pl.BlockSpec(memory_space=pl.ANY)
    smem = pl.BlockSpec(memory_space=pltpu.SMEM)
    scratch = [
        pltpu.VMEM((slots, 128, 128), BF16),
        pltpu.VMEM((slots, 128, 128), BF16),
        pltpu.VMEM((k0, local), F32),
        pltpu.VMEM((k0 * nt, 128), F32),
        pltpu.VMEM((nt, 128), F32),
        pltpu.VMEM((nt, 128), F32),
        pltpu.VMEM((64, 128), F32),
        pltpu.VMEM((64, 128), F32),
        pltpu.VMEM((64, 128), F32),
        pltpu.VMEM((64, 128), F32),
        pltpu.VMEM((64, 128), F32),
        pltpu.VMEM((128, local // 8), BF16),
        pltpu.VMEM((slots, 3 * subs * nt), BF16),
        pltpu.VMEM((subs * nt, slots), BF16),
        pltpu.VMEM((ITERS, 3 * subs, nt, 256), BF16),
        pltpu.VMEM((ITERS, subs, nt, 128), F32),
        pltpu.VMEM((ITERS, subs - 1, nt, 128), F32),
        pltpu.VMEM((128, 128), F32),
        pltpu.VMEM((ITERS, plan.plane, 1, 128), F32),
        pltpu.VMEM((ITERS, plan.line, 1, 128), F32),
        pltpu.VMEM((plan.plane, chunk, 128), F32),
        pltpu.VMEM((plan.plane, chunk, 128), F32),
        pltpu.VMEM((plan.line, chunk, 128), F32),
        pltpu.VMEM((plan.plane, chunk, 128), F32),
        pltpu.SemaphoreType.DMA((2,)),
        pltpu.SemaphoreType.DMA,
        pltpu.SemaphoreType.DMA((11,)),
        pltpu.SemaphoreType.DMA((11,)),
    ]
    outs = pl.pallas_call(
        functools.partial(body, plan, k0, j0, unknowns, slots, nt),
        out_shape=(
            jax.ShapeDtypeStruct((ITERS, local), F32),
            jax.ShapeDtypeStruct((2, k0 + ITERS, j0 + ITERS), F32),
            jax.ShapeDtypeStruct((j0 + ITERS, ITERS), F32),
        ),
        in_specs=[hbm, hbm, vmem, vmem, smem, hbm, vmem],
        out_specs=(vmem, vmem, vmem),
        scratch_shapes=scratch,
        compiler_params=pltpu.CompilerParams(
            collective_id=0, has_side_effects=True, vmem_limit_bytes=48 << 20
        ),
        name="toar",
    )(
        stiffness.reshape(stiffness.shape[2:]), damping.reshape(damping.shape[2:]),
        tile_map.reshape(2, slots), mass.reshape(nt, 128), shift.reshape(1), basis, compact,
    )
    return outs


def solution(mesh):
    rows, subs = mesh.shape["rows"], mesh.shape["sub"]
    both = ("rows", "sub")
    return jax.shard_map(
        functools.partial(on_device, rows=rows, subs=subs),
        mesh=mesh,
        in_specs=(
            P("rows", "sub", None, None, None), P("rows", "sub", None, None, None),
            P("rows", "sub", None, None), P(both), P(), P(None, both), P(),
        ),
        out_specs=(P(None, both), P(), P()),
        check_vma=False,
    )
```

```python
import functools
import itertools

import jax
import jax.numpy as jnp
from jax import lax
from jax.experimental import pallas as pl
from jax.experimental.pallas import tpu as pltpu
from jax.sharding import PartitionSpec as P

ITERS = 2
EPS = 1e-06
MESH = pl.DeviceIdType.MESH
F32 = jnp.float32
BF16 = jnp.bfloat16
HELD = 60


def dot_nt(a, b):
    return lax.dot_general(a, b, (((1,), (1,)), ((), ())), preferred_element_type=F32)


def halves(x):
    hi = x.astype(BF16)
    return hi, (x - hi.astype(F32)).astype(BF16)


def iota(shape, dim):
    return lax.broadcasted_iota(jnp.int32, shape, dim)


def lane_sum(x):
    return jnp.sum(x, axis=1, keepdims=True)


def row_sum(x):
    return jnp.sum(x, axis=0, keepdims=True)


def tree_sum(terms):
    while len(terms) > 1:
        terms = [sum(terms[i + 1 : i + 2], terms[i]) for i in range(0, len(terms), 2)]
    return terms[0]


def ring_distance(step, size):
    return min(step, size - step)


class Plan:
    def __init__(self, rows, subs):
        self.rows, self.subs = rows, subs
        self.cores = 2
        self.ys = 4 if rows >= 32 else 2
        self.zs = rows // (self.ys * self.cores)
        self.plane = self.ys * subs
        self.line = self.zs * self.cores
        self.cube = self.zs * self.ys * subs

    def steps(self, *sizes):
        every = [s for s in itertools.product(*map(range, sizes)) if any(s)]
        return sorted(every, key=lambda s: -sum(map(ring_distance, s, sizes)))


def body(
    plan, k0, j0, unknowns, slots, nt,
    stiff_hbm, damp_hbm, map_hbm, mass_hbm, shift_ref, basis_hbm, compact_hbm,
    new_ref, comp_ref, hess_ref,
    tiles_d, tiles_k, nat, held, map_s, mass_s, compact_s, image_s, column_s, coef_u, coef_l,
    square_s, upper_m, lower_m, gram_m, split_s, onehot_g, onehot_s, window, part_s, part_r,
    parts_m, pair_r, cube_r, gram_s, gram_1, gram_2, gram_3,
    copy_sem, send_sem, recv_sem, ready_sem,
):
    rows, subs = plan.rows, plan.subs
    basis_copy = pltpu.make_async_copy(basis_hbm, nat, copy_sem.at[0])
    basis_copy.start()

    row = lax.axis_index("rows")
    sub = lax.axis_index("sub")
    core = lax.rem(row, plan.cores)
    chip = lax.div(row, plan.cores)
    y = lax.rem(chip, plan.ys)
    z = lax.div(chip, plan.ys)
    in_plane = y * subs + sub
    in_line = z * plan.cores + core
    in_cube = chip * subs + sub
    to_x = [lax.rem(sub + i, subs) for i in range(subs)]
    to_y = [lax.rem(y + i, plan.ys) for i in range(plan.ys)]
    to_z = [lax.rem(z + i, plan.zs) for i in range(plan.zs)]
    to_c = [core, 1 - core]
    above = lax.rem(row + rows - 1, rows)
    below = lax.rem(row + 1, rows)

    def at(dz, dy, dc, dx):
        return ((to_z[dz] * plan.ys + to_y[dy]) * plan.cores + to_c[dc], to_x[dx])

    plane_peers = [
        (to_y[dy] * subs + to_x[dx], at(0, dy, 0, dx)) for dy, dx in plan.steps(plan.ys, subs)
    ]
    line_peers = [at(dz, 0, dc, 0) for dz, dc in plan.steps(plan.zs, plan.cores)]
    beside = [
        (device, to_x[dx])
        for dx in sorted(range(subs), key=lambda i: -ring_distance(i, subs))
        for device in (above, below)
    ]

    barrier = pltpu.get_barrier_semaphore()
    greeted = line_peers + beside + [device for _, device in plane_peers]
    for device in greeted:
        pl.semaphore_signal(barrier, inc=1, device_id=device, device_id_type=MESH)

    small = [
        pltpu.make_async_copy(compact_hbm, compact_s, copy_sem.at[1]),
        pltpu.make_async_copy(map_hbm, map_s, copy_sem.at[2]),
        pltpu.make_async_copy(mass_hbm, mass_s, copy_sem.at[3]),
    ]
    for copy in small:
        copy.start()

    def send(src, dst, which, device):
        pltpu.make_async_remote_copy(
            src_ref=src, dst_ref=dst, send_sem=send_sem.at[which], recv_sem=recv_sem.at[which],
            device_id=device, device_id_type=MESH,
        ).start()

    def arrived(view, which):
        pltpu.make_async_copy(view, view, recv_sem.at[which]).wait()

    def departed(view, which):
        pltpu.make_async_copy(view, view, send_sem.at[which]).wait()

    shift = shift_ref[0]
    scale = 1.0 / unknowns
    eye64 = (iota((64, 128), 0) == iota((64, 128), 1)).astype(F32)
    lane = iota((1, 128), 1)
    lane64 = iota((64, 128), 1)
    row64 = iota((64, 128), 0)
    column_s[...] = jnp.zeros_like(column_s)
    parts_m[...] = jnp.zeros_like(parts_m)
    split_s[...] = jnp.zeros_like(split_s)
    held[k0 * nt :, :] = jnp.zeros((held.shape[0] - k0 * nt, 128), F32)

    small[0].wait()
    for matrix, which in ((upper_m, 0), (lower_m, 1)):
        square_s[...] = jnp.zeros_like(square_s)
        square_s[0:j0, 0:k0] = compact_s[:, which, :]
        matrix[...] = square_s[...].T[0:64]
    comp_ref[...] = jnp.zeros_like(comp_ref)
    comp_ref[0:j0, :, 0:k0] = compact_s[...]
    u1 = jnp.broadcast_to(lane_sum(jnp.where(lane64 == j0 - 1, upper_m[...], 0.0)), (64, 128))
    u2 = jnp.broadcast_to(lane_sum(jnp.where(lane64 == j0 - 1, lower_m[...], 0.0)), (64, 128))
    coef_u[...] = u1
    coef_l[...] = u2

    basis_copy.wait()
    tile_copies = [
        pltpu.make_async_copy(damp_hbm, tiles_d, copy_sem.at[4]),
        pltpu.make_async_copy(stiff_hbm, tiles_k, copy_sem.at[5]),
    ]
    for copy in tile_copies:
        copy.start()

    def regroup(b, carry):
        for i in range(4):
            t = b * 4 + i
            held[pl.ds(t, k0, stride=nt), :] = nat[:, pl.ds(pl.multiple_of(t * 128, 128), 128)]
        return carry

    lax.fori_loop(0, nt // 4, regroup, 0)

    def combined(refs):
        def add(b, totals):
            for i in range(4):
                k = b * 4 + i
                h = held[pl.ds(pl.multiple_of(k * nt, 8), nt), :]
                totals = tuple(
                    total + h * jnp.broadcast_to(ref[pl.ds(k, 1), :], h.shape)
                    for total, ref in zip(totals, refs)
                )
            return totals
        return lax.fori_loop(0, HELD // 4, add, tuple(jnp.zeros((nt, 128), F32) for _ in refs))

    def pack(it, upper, lower):
        window[it, subs + sub] = jnp.concatenate([upper, lower], axis=1).astype(BF16)

    def exchange(it):
        mine = window.at[it, subs + sub]
        for device in beside:
            place = sub if device[0] is below else 2 * subs + sub
            send(mine, window.at[it, place], it, device)
        for step in range(1, subs):
            send(mine, mine, it, (row, to_x[step]))

    upper, lower = combined((coef_u, coef_l))
    pack(0, upper, lower)

    wide = nat.shape[1] // 8

    def gram_part(c, total):
        piece = nat[:, pl.ds(pl.multiple_of(c * wide, 128), wide)]
        hi, lo = halves(piece)
        split_s[0:k0, :] = hi
        split_s[64 : 64 + k0, :] = lo
        return total + dot_nt(split_s[...], split_s[0:64, :])

    def gram_ready():
        both = lax.fori_loop(0, 8, gram_part, jnp.zeros((128, 64), F32))
        cross = both[64:128]
        gram = both[0:64] + cross + cross.T
        gram = jnp.concatenate([gram, jnp.zeros((64, 64), F32)], axis=1)
        chunk = 64 // plan.plane
        for p in range(plan.plane):
            gram_s[p] = gram[p * chunk : (p + 1) * chunk]
        gram_1[in_plane] = gram_s[in_plane]

    small[1].wait()
    small[2].wait()
    target = map_s[0:1, :].astype(F32)
    source = map_s[1:2, :].astype(F32)
    onehot_s[...] = (
        jnp.broadcast_to(target, onehot_s.shape) == iota(onehot_s.shape, 0).astype(F32)
    ).astype(F32).astype(BF16)
    eye_s = (iota((slots, slots), 0) == iota((slots, slots), 1)).astype(F32)
    source_col = lane_sum(jnp.broadcast_to(source, (slots, slots)) * eye_s)
    spot = iota(onehot_g.shape, 1)
    first_tile = jnp.where(row == 0, subs * nt, 0)
    last_tile = jnp.where(row == rows - 1, 2 * subs * nt, 3 * subs * nt)
    hit = (
        (jnp.broadcast_to(source_col, onehot_g.shape) == spot.astype(F32))
        & (spot >= first_tile) & (spot < last_tile)
    )
    onehot_g[...] = hit.astype(F32).astype(BF16)
    gram_ready()

    pl.semaphore_wait(barrier, len(greeted))
    exchange(0)
    for _, device in plane_peers:
        pl.semaphore_signal(ready_sem, inc=1, device_id=device, device_id_type=MESH)
    for peer, device in plane_peers:
        send(gram_s.at[peer], gram_1.at[in_plane], 8, device)

    mass = mass_s[...]
    block = min(64, slots)
    lane_s = iota((128, slots), 1)
    plane_view = pl.ds(0, plan.plane - 1)
    line_view = pl.ds(0, plan.line - 1)
    cube_view = pl.ds(0, plan.cube - 1)

    for it in range(ITERS):
        m, cols = k0 + it, j0 + it
        arrived(window.at[it, pl.ds(0, 3 * subs - 1)], it)
        picked = jnp.dot(
            onehot_g[...], window[it].reshape(3 * subs * nt, 256), preferred_element_type=F32
        ).astype(BF16)
        if it == 0:
            for copy in tile_copies:
                copy.wait()

        def products(b, total):
            d = tiles_d[pl.ds(b * block, block)].reshape(block * 128, 128)
            k = tiles_k[pl.ds(b * block, block)].reshape(block * 128, 128)
            r = dot_nt(jnp.concatenate([d, k], axis=1), picked)
            for i in range(block):
                total = jnp.where(lane_s == b * block + i, r[i * 128 : (i + 1) * 128], total)
            return total

        product = lax.fori_loop(0, slots // block, products, jnp.zeros((128, slots), F32))
        hi, lo = halves(product)
        part = dot_nt(onehot_s[...], hi) + dot_nt(onehot_s[...], lo)
        part_s[it] = part.reshape(subs, nt, 128)
        for step in sorted(range(1, subs), key=lambda i: -ring_distance(i, subs)):
            send(part_s.at[it, to_x[step]], part_r.at[it, step - 1], 2 + it, (row, to_x[step]))
        if it == 0:
            arrived(gram_1.at[plane_view], 8)
            gram_2[in_line] = jnp.sum(gram_1[...], axis=0)
            for device in line_peers:
                send(gram_2.at[in_line], gram_2.at[in_line], 9, device)
        departed(window.at[it, pl.ds(0, 3 * subs - 1)], it)
        own = part_s[it, sub]
        arrived(part_r.at[it], 2 + it)
        coupled = own + part_r[it, 0]
        for step in range(2, subs):
            coupled = coupled + part_r[it, step - 1]
        image = shift * upper - mass * coupled
        image_s[...] = image

        def inner(b, total):
            for i in range(4):
                t = b * 4 + i
                piece = nat[:, pl.ds(pl.multiple_of(t * 128, 128), 128)]
                total = total + piece * jnp.broadcast_to(image_s[pl.ds(t, 1), :], piece.shape)
            return total

        parts_m[0:k0, :] = lax.fori_loop(0, nt // 4, inner, jnp.zeros((k0, 128), F32))
        if it > 0:
            parts_m[k0 : k0 + 1, :] = row_sum(column_s[...] * image)
        parts_m[63:64, :] = row_sum(image * image)
        pair_r[it, core] = row_sum(parts_m[...].T)
        send(pair_r.at[it, core], pair_r.at[it, core], 4 + it, at(0, 0, 1, 0))
        if it == 0:
            arrived(gram_2.at[line_view], 9)
            gram_3[in_plane] = jnp.sum(gram_2[...], axis=0)
            pl.semaphore_wait(ready_sem, plan.plane - 1)
        arrived(pair_r.at[it, 0], 4 + it)
        cube_r[it, in_cube] = pair_r[it, 0] + pair_r[it, 1]
        mine = cube_r.at[it, in_cube]
        for dz, dy, dx in plan.steps(plan.zs, plan.ys, subs):
            send(mine, mine, 6 + it, at(dz, dy, 0, dx))
        if it == 0:
            for _, device in plane_peers:
                send(gram_3.at[in_plane], gram_3.at[in_plane], 10, device)
        departed(part_r.at[it], 2 + it)
        departed(pair_r.at[it, 0], 4 + it)
        if it == 0:
            departed(gram_1.at[plane_view], 8)
            departed(gram_2.at[line_view], 9)
            departed(gram_3.at[plane_view], 10)
            arrived(gram_3.at[plane_view], 10)
            gram_m[...] = gram_3[...].reshape(64, 128) * scale
        gram = gram_m[...]
        turn = 2.0 * eye64 - gram
        up, low = upper_m[...], lower_m[...]
        lower_c = u1 + shift * u2
        arrived(cube_r.at[it, cube_view], 6 + it)
        sums = tree_sum([cube_r[it, i] for i in range(plan.cube)]) * scale

        own_square = lane_sum(jnp.where(lane == 63, sums, 0.0))
        first = jnp.where(lane < m, sums, 0.0)
        coef = jnp.broadcast_to(lane_sum(turn * first), (64, 128))
        coef_row = row_sum(eye64 * coef)
        gram_coef = row_sum(gram * coef)
        square = own_square + lane_sum(coef_row * (gram_coef - 2.0 * first))
        norm = jnp.sqrt(square + EPS)

        upper_c = jnp.where(row64 == m, norm, coef)
        weights = jnp.zeros((1, 128), F32)
        for _ in range(2):
            projection = row_sum(up * upper_c + low * lower_c)
            upper_c = upper_c - lane_sum(up * projection)
            lower_c = lower_c - lane_sum(low * projection)
            weights = weights + projection
        beta = jnp.sqrt(row_sum(upper_c * upper_c) + row_sum(lower_c * lower_c) + EPS)
        u1, u2 = upper_c / beta, lower_c / beta

        if it + 1 < ITERS:
            ratio = row_sum(jnp.where(row64 == m, u1, 0.0)) / norm
            coef_u[...] = u1 - ratio * coef
            coef_l[...] = u2
            held_u, lower = combined((coef_u, coef_l))
            upper = held_u + ratio * image
            pack(it + 1, upper, lower)
            exchange(it + 1)
            upper_m[...] = jnp.where(lane64 == cols, u1, up)
            lower_m[...] = jnp.where(lane64 == cols, u2, low)
        coef_u[...] = coef
        (taken,) = combined((coef_u,))
        column = (image - taken) / norm
        column_s[...] = column
        for t in range(nt):
            new_ref[it : it + 1, t * 128 : (t + 1) * 128] = column_s[t : t + 1, :]
        hess_ref[it : it + 1, :] = jnp.where(lane == cols, beta, weights)[:, 0 : j0 + ITERS]
        comp_ref[cols, 0:1, :] = row_sum(eye64 * u1)[:, 0 : k0 + ITERS]
        comp_ref[cols, 1:2, :] = row_sum(eye64 * u2)[:, 0 : k0 + ITERS]
        departed(cube_r.at[it, cube_view], 6 + it)
        if it + 1 < ITERS:
            held[m * nt : (m + 1) * nt, :] = column
            cross_row = (first - gram_coef) / norm
            cross_col = lane_sum(eye64 * cross_row)
            gram = jnp.where(row64 == m, cross_row, gram)
            gram = jnp.where(lane64 == m, cross_col, gram)
            gram = jnp.where((row64 == m) & (lane64 == m), square / (norm * norm), gram)
            gram_m[...] = gram


def put_out(*refs):
    ins, outs, sems = refs[:3], refs[3:6], refs[6]
    copies = [pltpu.make_async_copy(a, b, sems.at[i]) for i, (a, b) in enumerate(zip(ins, outs))]
    for copy in copies:
        copy.start()
    for copy in copies:
        copy.wait()


def on_device(stiffness, damping, tile_map, mass, shift, basis, compact, *, rows, subs):
    plan = Plan(rows, subs)
    k0, local = basis.shape
    j0 = compact.shape[2]
    slots = stiffness.shape[2]
    nt = local // 128
    unknowns = local * rows * subs
    chunk = 64 // plan.plane
    vmem = pl.BlockSpec(memory_space=pltpu.VMEM)
    hbm = pl.BlockSpec(memory_space=pltpu.HBM)
    smem = pl.BlockSpec(memory_space=pltpu.SMEM)
    scratch = [
        pltpu.VMEM((slots, 128, 128), BF16),
        pltpu.VMEM((slots, 128, 128), BF16),
        pltpu.VMEM((k0, local), F32),
        pltpu.VMEM((HELD * nt, 128), F32),
        pltpu.VMEM((2, slots), jnp.int32),
        pltpu.VMEM((nt, 128), F32),
        pltpu.VMEM((j0, 2, k0), F32),
        pltpu.VMEM((nt, 128), F32),
        pltpu.VMEM((nt, 128), F32),
        pltpu.VMEM((64, 128), F32),
        pltpu.VMEM((64, 128), F32),
        pltpu.VMEM((128, 128), F32),
        pltpu.VMEM((64, 128), F32),
        pltpu.VMEM((64, 128), F32),
        pltpu.VMEM((64, 128), F32),
        pltpu.VMEM((128, local // 8), BF16),
        pltpu.VMEM((slots, 3 * subs * nt), BF16),
        pltpu.VMEM((subs * nt, slots), BF16),
        pltpu.VMEM((ITERS, 3 * subs, nt, 256), BF16),
        pltpu.VMEM((ITERS, subs, nt, 128), F32),
        pltpu.VMEM((ITERS, subs - 1, nt, 128), F32),
        pltpu.VMEM((128, 128), F32),
        pltpu.VMEM((ITERS, 2, 1, 128), F32),
        pltpu.VMEM((ITERS, plan.cube, 1, 128), F32),
        pltpu.VMEM((plan.plane, chunk, 128), F32),
        pltpu.VMEM((plan.plane, chunk, 128), F32),
        pltpu.VMEM((plan.line, chunk, 128), F32),
        pltpu.VMEM((plan.plane, chunk, 128), F32),
        pltpu.SemaphoreType.DMA((6,)),
        pltpu.SemaphoreType.DMA((11,)),
        pltpu.SemaphoreType.DMA((11,)),
        pltpu.SemaphoreType.REGULAR,
    ]
    shapes = (
        jax.ShapeDtypeStruct((ITERS, local), F32),
        jax.ShapeDtypeStruct((j0 + ITERS, 2, k0 + ITERS), F32),
        jax.ShapeDtypeStruct((ITERS, j0 + ITERS), F32),
    )

    def pin(array):
        return pltpu.with_memory_space_constraint(array, pltpu.HBM)

    outs = pl.pallas_call(
        functools.partial(body, plan, k0, j0, unknowns, slots, nt),
        out_shape=shapes,
        in_specs=[hbm, hbm, hbm, hbm, smem, hbm, hbm],
        out_specs=(vmem, vmem, vmem),
        scratch_shapes=scratch,
        compiler_params=pltpu.CompilerParams(
            collective_id=0, has_side_effects=True, vmem_limit_bytes=48 << 20
        ),
        name="toar",
    )(
        pin(stiffness.reshape(stiffness.shape[2:])), pin(damping.reshape(damping.shape[2:])),
        pin(tile_map.reshape(2, slots)), pin(mass.reshape(nt, 128)), shift.reshape(1), pin(basis),
        pin(compact.transpose(2, 0, 1)),
    )
    new, comp, hess = pl.pallas_call(
        put_out,
        out_shape=shapes,
        in_specs=[vmem] * 3,
        out_specs=(hbm,) * 3,
        scratch_shapes=[pltpu.SemaphoreType.DMA((3,))],
        compiler_params=pltpu.CompilerParams(vmem_limit_bytes=2 << 20),
        name="put_out",
    )(*outs)
    return new, comp.transpose(1, 2, 0), hess.T


def solution(mesh):
    rows, subs = mesh.shape["rows"], mesh.shape["sub"]
    both = ("rows", "sub")
    return jax.shard_map(
        functools.partial(on_device, rows=rows, subs=subs),
        mesh=mesh,
        in_specs=(
            P("rows", "sub", None, None, None), P("rows", "sub", None, None, None),
            P("rows", "sub", None, None), P(both), P(), P(None, both), P(),
        ),
        out_specs=(P(None, both), P(), P()),
        check_vma=False,
    )
```

```python
import functools
import itertools

import jax
import jax.numpy as jnp
from jax import lax
from jax.experimental import pallas as pl
from jax.experimental.pallas import tpu as pltpu
from jax.sharding import PartitionSpec as P

ITERS = 2
EPS = 1e-06
MESH = pl.DeviceIdType.MESH
F32 = jnp.float32
BF16 = jnp.bfloat16
HELD = 60


def dot_nt(a, b):
    return lax.dot_general(a, b, (((1,), (1,)), ((), ())), preferred_element_type=F32)


def halves(x):
    hi = x.astype(BF16)
    return hi, (x - hi.astype(F32)).astype(BF16)


def iota(shape, dim):
    return lax.broadcasted_iota(jnp.int32, shape, dim)


def lane_sum(x):
    return jnp.sum(x, axis=1, keepdims=True)


def row_sum(x):
    return jnp.sum(x, axis=0, keepdims=True)


def tree_sum(terms):
    while len(terms) > 1:
        terms = [sum(terms[i + 1 : i + 2], terms[i]) for i in range(0, len(terms), 2)]
    return terms[0]


def ring_distance(step, size):
    return min(step, size - step)


class Plan:
    def __init__(self, rows, subs):
        self.rows, self.subs = rows, subs
        self.cores = 2
        self.ys = 4 if rows >= 32 else 2
        self.zs = rows // (self.ys * self.cores)
        self.plane = self.ys * subs
        self.line = self.zs * self.cores
        self.cube = self.zs * self.ys * subs

    def steps(self, *sizes):
        every = [s for s in itertools.product(*map(range, sizes)) if any(s)]
        return sorted(every, key=lambda s: -sum(map(ring_distance, s, sizes)))


def body(
    plan, k0, j0, unknowns, slots, nt,
    stiff_hbm, damp_hbm, map_hbm, mass_hbm, shift_ref, basis_hbm, compact_hbm,
    new_ref, comp_ref, hess_ref,
    tiles_d, tiles_k, nat, held, map_s, mass_s, compact_s, image_s, column_s, coef_u, coef_l,
    square_s, upper_m, lower_m, gram_m, split_s, onehot_g, onehot_s, window_l, window_u, part_s, part_r,
    parts_m, pair_r, cube_r, gram_s, gram_1, gram_2, gram_3,
    copy_sem, send_sem, recv_sem, ready_sem,
):
    rows, subs = plan.rows, plan.subs
    basis_copy = pltpu.make_async_copy(basis_hbm, nat, copy_sem.at[0])
    basis_copy.start()

    row = lax.axis_index("rows")
    sub = lax.axis_index("sub")
    core = lax.rem(row, plan.cores)
    chip = lax.div(row, plan.cores)
    y = lax.rem(chip, plan.ys)
    z = lax.div(chip, plan.ys)
    in_plane = y * subs + sub
    in_line = z * plan.cores + core
    in_cube = chip * subs + sub
    to_x = [lax.rem(sub + i, subs) for i in range(subs)]
    to_y = [lax.rem(y + i, plan.ys) for i in range(plan.ys)]
    to_z = [lax.rem(z + i, plan.zs) for i in range(plan.zs)]
    to_c = [core, 1 - core]
    above = lax.rem(row + rows - 1, rows)
    below = lax.rem(row + 1, rows)

    def at(dz, dy, dc, dx):
        return ((to_z[dz] * plan.ys + to_y[dy]) * plan.cores + to_c[dc], to_x[dx])

    plane_peers = [
        (to_y[dy] * subs + to_x[dx], at(0, dy, 0, dx)) for dy, dx in plan.steps(plan.ys, subs)
    ]
    line_peers = [at(dz, 0, dc, 0) for dz, dc in plan.steps(plan.zs, plan.cores)]
    beside = [
        (device, to_x[dx])
        for dx in sorted(range(subs), key=lambda i: -ring_distance(i, subs))
        for device in (above, below)
    ]

    barrier = pltpu.get_barrier_semaphore()
    greeted = line_peers + beside + [device for _, device in plane_peers]
    for device in greeted:
        pl.semaphore_signal(barrier, inc=1, device_id=device, device_id_type=MESH)

    small = [
        pltpu.make_async_copy(compact_hbm, compact_s, copy_sem.at[1]),
        pltpu.make_async_copy(map_hbm, map_s, copy_sem.at[2]),
        pltpu.make_async_copy(mass_hbm, mass_s, copy_sem.at[3]),
    ]
    for copy in small:
        copy.start()

    def send(src, dst, which, device):
        pltpu.make_async_remote_copy(
            src_ref=src, dst_ref=dst, send_sem=send_sem.at[which], recv_sem=recv_sem.at[which],
            device_id=device, device_id_type=MESH,
        ).start()

    def arrived(view, which):
        pltpu.make_async_copy(view, view, recv_sem.at[which]).wait()

    def departed(view, which):
        pltpu.make_async_copy(view, view, send_sem.at[which]).wait()

    shift = shift_ref[0]
    scale = 1.0 / unknowns
    eye64 = (iota((64, 128), 0) == iota((64, 128), 1)).astype(F32)
    lane = iota((1, 128), 1)
    lane64 = iota((64, 128), 1)
    row64 = iota((64, 128), 0)
    held[k0 * nt :, :] = jnp.zeros((held.shape[0] - k0 * nt, 128), F32)

    small[0].wait()
    last = compact_s[j0 - 1]
    last = jnp.concatenate([last, jnp.zeros((2, 128 - k0), F32)], axis=1)
    u1 = jnp.broadcast_to(lane_sum(eye64 * last[0:1]), (64, 128))
    u2 = jnp.broadcast_to(lane_sum(eye64 * last[1:2]), (64, 128))
    coef_u[...] = u1
    coef_l[...] = u2

    basis_copy.wait()
    tile_copies = [
        pltpu.make_async_copy(damp_hbm, tiles_d, copy_sem.at[4]),
        pltpu.make_async_copy(stiff_hbm, tiles_k, copy_sem.at[5]),
    ]
    for copy in tile_copies:
        copy.start()

    def regroup(b, carry):
        for i in range(4):
            t = b * 4 + i
            held[pl.ds(t, k0, stride=nt), :] = nat[:, pl.ds(pl.multiple_of(t * 128, 128), 128)]
        return carry

    lax.fori_loop(0, nt // 4, regroup, 0)

    def combined(ref):
        def add(b, total):
            for i in range(4):
                k = b * 4 + i
                h = held[pl.ds(pl.multiple_of(k * nt, 8), nt), :]
                total = total + h * jnp.broadcast_to(ref[pl.ds(k, 1), :], h.shape)
            return total
        return lax.fori_loop(0, HELD // 4, add, jnp.zeros((nt, 128), F32))

    def exchange(window, it, which, vector):
        mine = window.at[it, subs + sub]
        mine[...] = vector.astype(BF16)
        for device in beside:
            place = sub if device[0] is below else 2 * subs + sub
            send(mine, window.at[it, place], which, device)
        for step in sorted(range(1, subs), key=lambda i: -ring_distance(i, subs)):
            send(mine, mine, which, (row, to_x[step]))

    lower = combined(coef_l)
    pl.semaphore_wait(barrier, len(greeted))
    exchange(window_l, 0, 0, lower)
    upper = combined(coef_u)
    exchange(window_u, 0, 1, upper)
    for _, device in plane_peers:
        pl.semaphore_signal(ready_sem, inc=1, device_id=device, device_id_type=MESH)

    wide = nat.shape[1] // 8

    def gram_part(c, total):
        piece = nat[:, pl.ds(pl.multiple_of(c * wide, 128), wide)]
        hi, lo = halves(piece)
        split_s[0:k0, :] = hi
        split_s[64 : 64 + k0, :] = lo
        return total + dot_nt(split_s[...], split_s[0:64, :])

    def gram_ready():
        both = lax.fori_loop(0, 8, gram_part, jnp.zeros((128, 64), F32))
        cross = both[64:128]
        gram = both[0:64] + cross + cross.T
        gram = jnp.concatenate([gram, jnp.zeros((64, 64), F32)], axis=1)
        chunk = 64 // plan.plane
        for p in range(plan.plane):
            gram_s[p] = gram[p * chunk : (p + 1) * chunk]
        gram_1[in_plane] = gram_s[in_plane]

    column_s[...] = jnp.zeros_like(column_s)
    parts_m[...] = jnp.zeros_like(parts_m)
    split_s[...] = jnp.zeros_like(split_s)
    gram_ready()
    for peer, device in plane_peers:
        send(gram_s.at[peer], gram_1.at[in_plane], 10, device)

    for matrix, which in ((upper_m, 0), (lower_m, 1)):
        square_s[...] = jnp.zeros_like(square_s)
        square_s[0:j0, 0:k0] = compact_s[:, which, :]
        matrix[...] = square_s[...].T[0:64]
    comp_ref[...] = jnp.zeros_like(comp_ref)
    comp_ref[0:j0, :, 0:k0] = compact_s[...]

    small[1].wait()
    small[2].wait()
    target = map_s[0:1, :].astype(F32)
    source = map_s[1:2, :].astype(F32)
    onehot_s[...] = (
        jnp.broadcast_to(target, onehot_s.shape) == iota(onehot_s.shape, 0).astype(F32)
    ).astype(F32).astype(BF16)
    eye_s = (iota((slots, slots), 0) == iota((slots, slots), 1)).astype(F32)
    source_col = lane_sum(jnp.broadcast_to(source, (slots, slots)) * eye_s)
    spot = iota(onehot_g.shape, 1)
    first_tile = jnp.where(row == 0, subs * nt, 0)
    last_tile = jnp.where(row == rows - 1, 2 * subs * nt, 3 * subs * nt)
    hit = (
        (jnp.broadcast_to(source_col, onehot_g.shape) == spot.astype(F32))
        & (spot >= first_tile) & (spot < last_tile)
    )
    onehot_g[...] = hit.astype(F32).astype(BF16)

    mass = mass_s[...]
    block = min(64, slots)
    pair_s = lax.div(iota((128, slots), 1), 2)
    even_s = lax.rem(iota((slots, 128), 0), 2) == 0
    others = pl.ds(0, 3 * subs - 1)
    plane_view = pl.ds(0, plan.plane - 1)
    line_view = pl.ds(0, plan.line - 1)
    cube_view = pl.ds(0, plan.cube - 1)

    for it in range(ITERS):
        m, cols = k0 + it, j0 + it
        def products(tiles, window, which):
            arrived(window.at[it, others], which)
            source = window[it].reshape(3 * subs * nt, 128)
            picked = jnp.dot(onehot_g[...], source, preferred_element_type=F32)
            even = jnp.where(even_s, picked, 0.0)
            picked = jnp.concatenate([even, picked - even], axis=1).astype(BF16)

            def some(b, total):
                t = tiles[pl.ds(b * block, block)].reshape(block // 2, 2, 128, 128)
                pairs = jnp.concatenate([t[:, 0], t[:, 1]], axis=2).reshape(block * 64, 256)
                r = dot_nt(pairs, picked)
                for i in range(block // 2):
                    here = pair_s == b * (block // 2) + i
                    total = jnp.where(here, r[i * 128 : (i + 1) * 128], total)
                return total

            return lax.fori_loop(0, slots // block, some, jnp.zeros((128, slots), F32))

        if it == 0:
            for copy in tile_copies:
                copy.wait()
        product = products(tiles_k, window_l, 2 * it)
        product = product + products(tiles_d, window_u, 2 * it + 1)
        hi, lo = halves(product)
        part = dot_nt(onehot_s[...], hi) + dot_nt(onehot_s[...], lo)
        part_s[it] = part.reshape(subs, nt, 128)
        for step in sorted(range(1, subs), key=lambda i: -ring_distance(i, subs)):
            send(part_s.at[it, to_x[step]], part_r.at[it, step - 1], 4 + it, (row, to_x[step]))
        if it == 0:
            arrived(gram_1.at[plane_view], 10)
            gram_2[in_line] = jnp.sum(gram_1[...], axis=0)
            for device in line_peers:
                send(gram_2.at[in_line], gram_2.at[in_line], 11, device)
        departed(window_l.at[it, others], 2 * it)
        departed(window_u.at[it, others], 2 * it + 1)
        own = part_s[it, sub]
        arrived(part_r.at[it], 4 + it)
        coupled = own + part_r[it, 0]
        for step in range(2, subs):
            coupled = coupled + part_r[it, step - 1]
        image = shift * upper - mass * coupled
        image_s[...] = image

        def inner(b, total):
            for i in range(4):
                t = b * 4 + i
                piece = nat[:, pl.ds(pl.multiple_of(t * 128, 128), 128)]
                total = total + piece * jnp.broadcast_to(image_s[pl.ds(t, 1), :], piece.shape)
            return total

        parts_m[0:k0, :] = lax.fori_loop(0, nt // 4, inner, jnp.zeros((k0, 128), F32))
        if it > 0:
            parts_m[k0 : k0 + 1, :] = row_sum(column_s[...] * image)
        parts_m[63:64, :] = row_sum(image * image)
        pair_r[it, core] = row_sum(parts_m[...].T)
        send(pair_r.at[it, core], pair_r.at[it, core], 6 + it, at(0, 0, 1, 0))
        if it == 0:
            arrived(gram_2.at[line_view], 11)
            gram_3[in_plane] = jnp.sum(gram_2[...], axis=0)
            pl.semaphore_wait(ready_sem, plan.plane - 1)
        arrived(pair_r.at[it, 0], 6 + it)
        cube_r[it, in_cube] = pair_r[it, 0] + pair_r[it, 1]
        mine = cube_r.at[it, in_cube]
        for dz, dy, dx in plan.steps(plan.zs, plan.ys, subs):
            send(mine, mine, 8 + it, at(dz, dy, 0, dx))
        if it == 0:
            for _, device in plane_peers:
                send(gram_3.at[in_plane], gram_3.at[in_plane], 12, device)
        departed(part_r.at[it], 4 + it)
        departed(pair_r.at[it, 0], 6 + it)
        if it == 0:
            departed(gram_1.at[plane_view], 10)
            departed(gram_2.at[line_view], 11)
            departed(gram_3.at[plane_view], 12)
            arrived(gram_3.at[plane_view], 12)
            gram_m[...] = gram_3[...].reshape(64, 128) * scale
        gram = gram_m[...]
        turn = 2.0 * eye64 - gram
        up, low = upper_m[...], lower_m[...]
        lower_c = u1 + shift * u2
        arrived(cube_r.at[it, cube_view], 8 + it)
        sums = tree_sum([cube_r[it, i] for i in range(plan.cube)]) * scale

        own_square = lane_sum(jnp.where(lane == 63, sums, 0.0))
        first = jnp.where(lane < m, sums, 0.0)
        coef = jnp.broadcast_to(lane_sum(turn * first), (64, 128))
        coef_row = row_sum(eye64 * coef)
        gram_coef = row_sum(gram * coef)
        square = own_square + lane_sum(coef_row * (gram_coef - 2.0 * first))
        norm = jnp.sqrt(square + EPS)

        upper_c = jnp.where(row64 == m, norm, coef)
        weights = jnp.zeros((1, 128), F32)
        for _ in range(2):
            projection = row_sum(up * upper_c + low * lower_c)
            upper_c = upper_c - lane_sum(up * projection)
            lower_c = lower_c - lane_sum(low * projection)
            weights = weights + projection
        beta = jnp.sqrt(row_sum(upper_c * upper_c) + row_sum(lower_c * lower_c) + EPS)
        u1, u2 = upper_c / beta, lower_c / beta

        if it + 1 < ITERS:
            ratio = row_sum(jnp.where(row64 == m, u1, 0.0)) / norm
            coef_u[...] = u1 - ratio * coef
            coef_l[...] = u2
            exchange(window_l, it + 1, 2 * it + 2, combined(coef_l))
            upper = combined(coef_u) + ratio * image
            exchange(window_u, it + 1, 2 * it + 3, upper)
            upper_m[...] = jnp.where(lane64 == cols, u1, up)
            lower_m[...] = jnp.where(lane64 == cols, u2, low)
        coef_u[...] = coef
        column = (image - combined(coef_u)) / norm
        column_s[...] = column
        for t in range(nt):
            new_ref[it : it + 1, t * 128 : (t + 1) * 128] = column_s[t : t + 1, :]
        hess_ref[it : it + 1, :] = jnp.where(lane == cols, beta, weights)[:, 0 : j0 + ITERS]
        comp_ref[cols, 0:1, :] = row_sum(eye64 * u1)[:, 0 : k0 + ITERS]
        comp_ref[cols, 1:2, :] = row_sum(eye64 * u2)[:, 0 : k0 + ITERS]
        departed(cube_r.at[it, cube_view], 8 + it)
        if it + 1 < ITERS:
            held[m * nt : (m + 1) * nt, :] = column
            cross_row = (first - gram_coef) / norm
            cross_col = lane_sum(eye64 * cross_row)
            gram = jnp.where(row64 == m, cross_row, gram)
            gram = jnp.where(lane64 == m, cross_col, gram)
            gram = jnp.where((row64 == m) & (lane64 == m), square / (norm * norm), gram)
            gram_m[...] = gram


def put_out(*refs):
    ins, outs, sems = refs[:3], refs[3:6], refs[6]
    copies = [pltpu.make_async_copy(a, b, sems.at[i]) for i, (a, b) in enumerate(zip(ins, outs))]
    for copy in copies:
        copy.start()
    for copy in copies:
        copy.wait()


def on_device(stiffness, damping, tile_map, mass, shift, basis, compact, *, rows, subs):
    plan = Plan(rows, subs)
    k0, local = basis.shape
    j0 = compact.shape[2]
    slots = stiffness.shape[2]
    nt = local // 128
    unknowns = local * rows * subs
    chunk = 64 // plan.plane
    vmem = pl.BlockSpec(memory_space=pltpu.VMEM)
    hbm = pl.BlockSpec(memory_space=pltpu.HBM)
    smem = pl.BlockSpec(memory_space=pltpu.SMEM)
    scratch = [
        pltpu.VMEM((slots, 128, 128), BF16),
        pltpu.VMEM((slots, 128, 128), BF16),
        pltpu.VMEM((k0, local), F32),
        pltpu.VMEM((HELD * nt, 128), F32),
        pltpu.VMEM((2, slots), jnp.int32),
        pltpu.VMEM((nt, 128), F32),
        pltpu.VMEM((j0, 2, k0), F32),
        pltpu.VMEM((nt, 128), F32),
        pltpu.VMEM((nt, 128), F32),
        pltpu.VMEM((64, 128), F32),
        pltpu.VMEM((64, 128), F32),
        pltpu.VMEM((128, 128), F32),
        pltpu.VMEM((64, 128), F32),
        pltpu.VMEM((64, 128), F32),
        pltpu.VMEM((64, 128), F32),
        pltpu.VMEM((128, local // 8), BF16),
        pltpu.VMEM((slots, 3 * subs * nt), BF16),
        pltpu.VMEM((subs * nt, slots), BF16),
        pltpu.VMEM((ITERS, 3 * subs, nt, 128), BF16),
        pltpu.VMEM((ITERS, 3 * subs, nt, 128), BF16),
        pltpu.VMEM((ITERS, subs, nt, 128), F32),
        pltpu.VMEM((ITERS, subs - 1, nt, 128), F32),
        pltpu.VMEM((128, 128), F32),
        pltpu.VMEM((ITERS, 2, 1, 128), F32),
        pltpu.VMEM((ITERS, plan.cube, 1, 128), F32),
        pltpu.VMEM((plan.plane, chunk, 128), F32),
        pltpu.VMEM((plan.plane, chunk, 128), F32),
        pltpu.VMEM((plan.line, chunk, 128), F32),
        pltpu.VMEM((plan.plane, chunk, 128), F32),
        pltpu.SemaphoreType.DMA((6,)),
        pltpu.SemaphoreType.DMA((13,)),
        pltpu.SemaphoreType.DMA((13,)),
        pltpu.SemaphoreType.REGULAR,
    ]
    shapes = (
        jax.ShapeDtypeStruct((ITERS, local), F32),
        jax.ShapeDtypeStruct((j0 + ITERS, 2, k0 + ITERS), F32),
        jax.ShapeDtypeStruct((ITERS, j0 + ITERS), F32),
    )

    def pin(array):
        return pltpu.with_memory_space_constraint(array, pltpu.HBM)

    outs = pl.pallas_call(
        functools.partial(body, plan, k0, j0, unknowns, slots, nt),
        out_shape=shapes,
        in_specs=[hbm, hbm, hbm, hbm, smem, hbm, hbm],
        out_specs=(vmem, vmem, vmem),
        scratch_shapes=scratch,
        compiler_params=pltpu.CompilerParams(
            collective_id=0, has_side_effects=True, vmem_limit_bytes=48 << 20
        ),
        name="toar",
    )(
        pin(stiffness.reshape(stiffness.shape[2:])), pin(damping.reshape(damping.shape[2:])),
        pin(tile_map.reshape(2, slots)), pin(mass.reshape(nt, 128)), shift.reshape(1), pin(basis),
        pin(compact.transpose(2, 0, 1)),
    )
    new, comp, hess = pl.pallas_call(
        put_out,
        out_shape=shapes,
        in_specs=[vmem] * 3,
        out_specs=(hbm,) * 3,
        scratch_shapes=[pltpu.SemaphoreType.DMA((3,))],
        compiler_params=pltpu.CompilerParams(vmem_limit_bytes=2 << 20),
        name="put_out",
    )(*outs)
    return new, comp.transpose(1, 2, 0), hess.T


def solution(mesh):
    rows, subs = mesh.shape["rows"], mesh.shape["sub"]
    both = ("rows", "sub")
    return jax.shard_map(
        functools.partial(on_device, rows=rows, subs=subs),
        mesh=mesh,
        in_specs=(
            P("rows", "sub", None, None, None), P("rows", "sub", None, None, None),
            P("rows", "sub", None, None), P(both), P(), P(None, both), P(),
        ),
        out_specs=(P(None, both), P(), P()),
        check_vma=False,
    )
```

```python
import functools
import itertools

import jax
import jax.numpy as jnp
from jax import lax
from jax.experimental import pallas as pl
from jax.experimental.pallas import tpu as pltpu
from jax.sharding import PartitionSpec as P

ITERS = 2
EPS = 1e-06
MESH = pl.DeviceIdType.MESH
F32 = jnp.float32
BF16 = jnp.bfloat16
HELD = 60


def dot_nt(a, b):
    return lax.dot_general(a, b, (((1,), (1,)), ((), ())), preferred_element_type=F32)


def halves(x):
    hi = x.astype(BF16)
    return hi, (x - hi.astype(F32)).astype(BF16)


def iota(shape, dim):
    return lax.broadcasted_iota(jnp.int32, shape, dim)


def lane_sum(x):
    return jnp.sum(x, axis=1, keepdims=True)


def row_sum(x):
    return jnp.sum(x, axis=0, keepdims=True)


def tree_sum(terms):
    while len(terms) > 1:
        terms = [sum(terms[i + 1 : i + 2], terms[i]) for i in range(0, len(terms), 2)]
    return terms[0]


def ring_distance(step, size):
    return min(step, size - step)


class Plan:
    def __init__(self, rows, subs):
        self.rows, self.subs = rows, subs
        self.cores = 2
        self.ys = 4 if rows >= 32 else 2
        self.zs = rows // (self.ys * self.cores)
        self.plane = self.ys * subs
        self.line = self.zs * self.cores
        self.cube = self.zs * self.ys * subs

    def steps(self, *sizes):
        every = [s for s in itertools.product(*map(range, sizes)) if any(s)]
        return sorted(every, key=lambda s: -sum(map(ring_distance, s, sizes)))


def body(
    plan, k0, j0, unknowns, slots, nt,
    stiff_hbm, damp_hbm, map_hbm, mass_hbm, shift_ref, basis_hbm, compact_hbm,
    new_ref, comp_ref, hess_ref,
    tiles_d, tiles_k, nat, held, map_s, mass_s, compact_s, image_s, column_s, coef_u, coef_l,
    square_s, upper_m, lower_m, gram_m, split_s, onehot_g, onehot_s, window_l, window_u, part_f, part_s, part_r,
    parts_m, pair_r, cube_r, gram_s, gram_1, gram_2, gram_3,
    copy_sem, send_sem, recv_sem, ready_sem,
):
    rows, subs = plan.rows, plan.subs
    basis_copy = pltpu.make_async_copy(basis_hbm, nat, copy_sem.at[0])
    basis_copy.start()

    row = lax.axis_index("rows")
    sub = lax.axis_index("sub")
    core = lax.rem(row, plan.cores)
    chip = lax.div(row, plan.cores)
    y = lax.rem(chip, plan.ys)
    z = lax.div(chip, plan.ys)
    in_plane = y * subs + sub
    in_line = z * plan.cores + core
    in_cube = chip * subs + sub
    to_x = [lax.rem(sub + i, subs) for i in range(subs)]
    to_y = [lax.rem(y + i, plan.ys) for i in range(plan.ys)]
    to_z = [lax.rem(z + i, plan.zs) for i in range(plan.zs)]
    to_c = [core, 1 - core]
    above = lax.rem(row + rows - 1, rows)
    below = lax.rem(row + 1, rows)

    def at(dz, dy, dc, dx):
        return ((to_z[dz] * plan.ys + to_y[dy]) * plan.cores + to_c[dc], to_x[dx])

    plane_peers = [
        (to_y[dy] * subs + to_x[dx], at(0, dy, 0, dx)) for dy, dx in plan.steps(plan.ys, subs)
    ]
    line_peers = [at(dz, 0, dc, 0) for dz, dc in plan.steps(plan.zs, plan.cores)]
    beside = [
        (device, to_x[dx])
        for dx in sorted(range(subs), key=lambda i: -ring_distance(i, subs))
        for device in (above, below)
    ]

    barrier = pltpu.get_barrier_semaphore()
    greeted = line_peers + beside + [device for _, device in plane_peers]
    for device in greeted:
        pl.semaphore_signal(barrier, inc=1, device_id=device, device_id_type=MESH)

    small = [
        pltpu.make_async_copy(compact_hbm, compact_s, copy_sem.at[1]),
        pltpu.make_async_copy(map_hbm, map_s, copy_sem.at[2]),
        pltpu.make_async_copy(mass_hbm, mass_s, copy_sem.at[3]),
    ]
    for copy in small:
        copy.start()

    def send(src, dst, which, device):
        pltpu.make_async_remote_copy(
            src_ref=src, dst_ref=dst, send_sem=send_sem.at[which], recv_sem=recv_sem.at[which],
            device_id=device, device_id_type=MESH,
        ).start()

    def arrived(view, which):
        pltpu.make_async_copy(view, view, recv_sem.at[which]).wait()

    def departed(view, which):
        pltpu.make_async_copy(view, view, send_sem.at[which]).wait()

    shift = shift_ref[0]
    scale = 1.0 / unknowns
    eye64 = (iota((64, 128), 0) == iota((64, 128), 1)).astype(F32)
    lane = iota((1, 128), 1)
    lane64 = iota((64, 128), 1)
    row64 = iota((64, 128), 0)
    held[k0 * nt :, :] = jnp.zeros((held.shape[0] - k0 * nt, 128), F32)

    small[0].wait()
    last = compact_s[j0 - 1]
    last = jnp.concatenate([last, jnp.zeros((2, 128 - k0), F32)], axis=1)
    u1 = jnp.broadcast_to(lane_sum(eye64 * last[0:1]), (64, 128))
    u2 = jnp.broadcast_to(lane_sum(eye64 * last[1:2]), (64, 128))
    coef_u[...] = u1
    coef_l[...] = u2

    basis_copy.wait()
    tile_copies = [
        pltpu.make_async_copy(damp_hbm, tiles_d, copy_sem.at[4]),
        pltpu.make_async_copy(stiff_hbm, tiles_k, copy_sem.at[5]),
    ]
    for copy in tile_copies:
        copy.start()

    def regroup(b, carry):
        for i in range(4):
            t = b * 4 + i
            held[pl.ds(t, k0, stride=nt), :] = nat[:, pl.ds(pl.multiple_of(t * 128, 128), 128)]
        return carry

    lax.fori_loop(0, nt // 4, regroup, 0)

    def combined(ref):
        def add(b, total):
            for i in range(12):
                k = b * 12 + i
                h = held[pl.ds(pl.multiple_of(k * nt, 8), nt), :]
                total = total + h * jnp.broadcast_to(ref[pl.ds(k, 1), :], h.shape)
            return total
        return lax.fori_loop(0, HELD // 12, add, jnp.zeros((nt, 128), F32))

    def exchange(window, it, which, vector):
        mine = window.at[it, subs + sub]
        mine[...] = vector.astype(BF16)
        for device in beside:
            place = sub if device[0] is below else 2 * subs + sub
            send(mine, window.at[it, place], which, device)
        for step in sorted(range(1, subs), key=lambda i: -ring_distance(i, subs)):
            send(mine, mine, which, (row, to_x[step]))

    lower = combined(coef_l)
    pl.semaphore_wait(barrier, len(greeted))
    exchange(window_l, 0, 0, lower)
    upper = combined(coef_u)
    exchange(window_u, 0, 1, upper)
    for _, device in plane_peers:
        pl.semaphore_signal(ready_sem, inc=1, device_id=device, device_id_type=MESH)

    wide = nat.shape[1] // 8

    def gram_part(c, total):
        piece = nat[:, pl.ds(pl.multiple_of(c * wide, 128), wide)]
        hi, lo = halves(piece)
        split_s[0:k0, :] = hi
        split_s[64 : 64 + k0, :] = lo
        return total + dot_nt(split_s[...], split_s[0:64, :])

    def gram_ready():
        both = lax.fori_loop(0, 8, gram_part, jnp.zeros((128, 64), F32))
        cross = both[64:128]
        gram = both[0:64] + cross + cross.T
        gram = jnp.concatenate([gram, jnp.zeros((64, 64), F32)], axis=1)
        chunk = 64 // plan.plane
        for p in range(plan.plane):
            gram_s[p] = gram[p * chunk : (p + 1) * chunk]
        gram_1[in_plane] = gram_s[in_plane]

    column_s[...] = jnp.zeros_like(column_s)
    parts_m[...] = jnp.zeros_like(parts_m)
    split_s[...] = jnp.zeros_like(split_s)
    gram_ready()
    for peer, device in plane_peers:
        send(gram_s.at[peer], gram_1.at[in_plane], 10, device)

    for matrix, which in ((upper_m, 0), (lower_m, 1)):
        square_s[...] = jnp.zeros_like(square_s)
        square_s[0:j0, 0:k0] = compact_s[:, which, :]
        matrix[...] = square_s[...].T[0:64]
    comp_ref[...] = jnp.zeros_like(comp_ref)
    comp_ref[0:j0, :, 0:k0] = compact_s[...]

    small[1].wait()
    small[2].wait()
    target = map_s[0:1, :].astype(F32)
    source = map_s[1:2, :].astype(F32)
    onehot_s[...] = (
        jnp.broadcast_to(target, onehot_s.shape) == iota(onehot_s.shape, 0).astype(F32)
    ).astype(F32).astype(BF16)
    eye_s = (iota((slots, slots), 0) == iota((slots, slots), 1)).astype(F32)
    source_col = lane_sum(jnp.broadcast_to(source, (slots, slots)) * eye_s)
    spot = iota(onehot_g.shape, 1)
    first_tile = jnp.where(row == 0, subs * nt, 0)
    last_tile = jnp.where(row == rows - 1, 2 * subs * nt, 3 * subs * nt)
    hit = (
        (jnp.broadcast_to(source_col, onehot_g.shape) == spot.astype(F32))
        & (spot >= first_tile) & (spot < last_tile)
    )
    onehot_g[...] = hit.astype(F32).astype(BF16)

    mass = mass_s[...]
    block = min(64, slots)
    pair_s = lax.div(iota((128, slots), 1), 2)
    even_s = lax.rem(iota((slots, 128), 0), 2) == 0
    others = pl.ds(0, 3 * subs - 1)
    plane_view = pl.ds(0, plan.plane - 1)
    line_view = pl.ds(0, plan.line - 1)
    cube_view = pl.ds(0, plan.cube - 1)

    for it in range(ITERS):
        m, cols = k0 + it, j0 + it
        def products(tiles, window, which):
            arrived(window.at[it, others], which)
            source = window[it].reshape(3 * subs * nt, 128)
            picked = jnp.dot(onehot_g[...], source, preferred_element_type=F32)
            even = jnp.where(even_s, picked, 0.0)
            picked = jnp.concatenate([even, picked - even], axis=1).astype(BF16)

            def some(b, total):
                t = tiles[pl.ds(b * block, block)].reshape(block // 2, 2, 128, 128)
                pairs = jnp.concatenate([t[:, 0], t[:, 1]], axis=2).reshape(block * 64, 256)
                r = dot_nt(pairs, picked)
                for i in range(block // 2):
                    here = pair_s == b * (block // 2) + i
                    total = jnp.where(here, r[i * 128 : (i + 1) * 128], total)
                return total

            return lax.fori_loop(0, slots // block, some, jnp.zeros((128, slots), F32))

        if it == 0:
            for copy in tile_copies:
                copy.wait()
        product = products(tiles_k, window_l, 2 * it)
        product = product + products(tiles_d, window_u, 2 * it + 1)
        hi, lo = halves(product)
        part = dot_nt(onehot_s[...], hi) + dot_nt(onehot_s[...], lo)
        part_f[...] = part.reshape(subs, nt, 128)
        part_s[it] = part.reshape(subs, nt, 128).astype(BF16)
        for step in sorted(range(1, subs), key=lambda i: -ring_distance(i, subs)):
            send(part_s.at[it, to_x[step]], part_r.at[it, step - 1], 4 + it, (row, to_x[step]))
        if it == 0:
            arrived(gram_1.at[plane_view], 10)
            gram_2[in_line] = jnp.sum(gram_1[...], axis=0)
            for device in line_peers:
                send(gram_2.at[in_line], gram_2.at[in_line], 11, device)
        departed(window_l.at[it, others], 2 * it)
        departed(window_u.at[it, others], 2 * it + 1)
        own = part_f[sub]
        arrived(part_r.at[it], 4 + it)
        coupled = own
        for step in range(1, subs):
            coupled = coupled + part_r[it, step - 1].astype(F32)
        image = shift * upper - mass * coupled
        image_s[...] = image

        def inner(b, total):
            for i in range(8):
                t = b * 8 + i
                piece = nat[:, pl.ds(pl.multiple_of(t * 128, 128), 128)]
                total = total + piece * jnp.broadcast_to(image_s[pl.ds(t, 1), :], piece.shape)
            return total

        parts_m[0:k0, :] = lax.fori_loop(0, nt // 8, inner, jnp.zeros((k0, 128), F32))
        if it > 0:
            parts_m[k0 : k0 + 1, :] = row_sum(column_s[...] * image)
        parts_m[63:64, :] = row_sum(image * image)
        pair_r[it, core] = row_sum(parts_m[...].T)
        send(pair_r.at[it, core], pair_r.at[it, core], 6 + it, at(0, 0, 1, 0))
        if it == 0:
            arrived(gram_2.at[line_view], 11)
            gram_3[in_plane] = jnp.sum(gram_2[...], axis=0)
            pl.semaphore_wait(ready_sem, plan.plane - 1)
        arrived(pair_r.at[it, 0], 6 + it)
        cube_r[it, in_cube] = pair_r[it, 0] + pair_r[it, 1]
        mine = cube_r.at[it, in_cube]
        for dz, dy, dx in plan.steps(plan.zs, plan.ys, subs):
            send(mine, mine, 8 + it, at(dz, dy, 0, dx))
        if it == 0:
            for _, device in plane_peers:
                send(gram_3.at[in_plane], gram_3.at[in_plane], 12, device)
        departed(part_r.at[it], 4 + it)
        departed(pair_r.at[it, 0], 6 + it)
        if it == 0:
            departed(gram_1.at[plane_view], 10)
            departed(gram_2.at[line_view], 11)
            departed(gram_3.at[plane_view], 12)
            arrived(gram_3.at[plane_view], 12)
            gram_m[...] = gram_3[...].reshape(64, 128) * scale
        gram = gram_m[...]
        turn = 2.0 * eye64 - gram
        up, low = upper_m[...], lower_m[...]
        lower_c = u1 + shift * u2
        arrived(cube_r.at[it, cube_view], 8 + it)
        sums = tree_sum([cube_r[it, i] for i in range(plan.cube)]) * scale

        own_square = lane_sum(jnp.where(lane == 63, sums, 0.0))
        first = jnp.where(lane < m, sums, 0.0)
        coef = jnp.broadcast_to(lane_sum(turn * first), (64, 128))
        coef_row = row_sum(eye64 * coef)
        gram_coef = row_sum(gram * coef)
        square = own_square + lane_sum(coef_row * (gram_coef - 2.0 * first))
        norm = jnp.sqrt(square + EPS)

        upper_c = jnp.where(row64 == m, norm, coef)
        weights = jnp.zeros((1, 128), F32)
        for _ in range(2):
            projection = row_sum(up * upper_c + low * lower_c)
            upper_c = upper_c - lane_sum(up * projection)
            lower_c = lower_c - lane_sum(low * projection)
            weights = weights + projection
        beta = jnp.sqrt(row_sum(upper_c * upper_c) + row_sum(lower_c * lower_c) + EPS)
        u1, u2 = upper_c / beta, lower_c / beta

        if it + 1 < ITERS:
            ratio = row_sum(jnp.where(row64 == m, u1, 0.0)) / norm
            coef_u[...] = u1 - ratio * coef
            coef_l[...] = u2
            exchange(window_l, it + 1, 2 * it + 2, combined(coef_l))
            upper = combined(coef_u) + ratio * image
            exchange(window_u, it + 1, 2 * it + 3, upper)
            upper_m[...] = jnp.where(lane64 == cols, u1, up)
            lower_m[...] = jnp.where(lane64 == cols, u2, low)
        coef_u[...] = coef
        column = (image - combined(coef_u)) / norm
        column_s[...] = column
        for t in range(nt):
            new_ref[it : it + 1, t * 128 : (t + 1) * 128] = column_s[t : t + 1, :]
        hess_ref[it : it + 1, :] = jnp.where(lane == cols, beta, weights)[:, 0 : j0 + ITERS]
        comp_ref[cols, 0:1, :] = row_sum(eye64 * u1)[:, 0 : k0 + ITERS]
        comp_ref[cols, 1:2, :] = row_sum(eye64 * u2)[:, 0 : k0 + ITERS]
        departed(cube_r.at[it, cube_view], 8 + it)
        if it + 1 < ITERS:
            held[m * nt : (m + 1) * nt, :] = column
            cross_row = (first - gram_coef) / norm
            cross_col = lane_sum(eye64 * cross_row)
            gram = jnp.where(row64 == m, cross_row, gram)
            gram = jnp.where(lane64 == m, cross_col, gram)
            gram = jnp.where((row64 == m) & (lane64 == m), square / (norm * norm), gram)
            gram_m[...] = gram


def put_out(*refs):
    ins, outs, sems = refs[:3], refs[3:6], refs[6]
    copies = [pltpu.make_async_copy(a, b, sems.at[i]) for i, (a, b) in enumerate(zip(ins, outs))]
    for copy in copies:
        copy.start()
    for copy in copies:
        copy.wait()


def on_device(stiffness, damping, tile_map, mass, shift, basis, compact, *, rows, subs):
    plan = Plan(rows, subs)
    k0, local = basis.shape
    j0 = compact.shape[2]
    slots = stiffness.shape[2]
    nt = local // 128
    unknowns = local * rows * subs
    chunk = 64 // plan.plane
    vmem = pl.BlockSpec(memory_space=pltpu.VMEM)
    hbm = pl.BlockSpec(memory_space=pltpu.HBM)
    smem = pl.BlockSpec(memory_space=pltpu.SMEM)
    scratch = [
        pltpu.VMEM((slots, 128, 128), BF16),
        pltpu.VMEM((slots, 128, 128), BF16),
        pltpu.VMEM((k0, local), F32),
        pltpu.VMEM((HELD * nt, 128), F32),
        pltpu.VMEM((2, slots), jnp.int32),
        pltpu.VMEM((nt, 128), F32),
        pltpu.VMEM((j0, 2, k0), F32),
        pltpu.VMEM((nt, 128), F32),
        pltpu.VMEM((nt, 128), F32),
        pltpu.VMEM((64, 128), F32),
        pltpu.VMEM((64, 128), F32),
        pltpu.VMEM((128, 128), F32),
        pltpu.VMEM((64, 128), F32),
        pltpu.VMEM((64, 128), F32),
        pltpu.VMEM((64, 128), F32),
        pltpu.VMEM((128, local // 8), BF16),
        pltpu.VMEM((slots, 3 * subs * nt), BF16),
        pltpu.VMEM((subs * nt, slots), BF16),
        pltpu.VMEM((ITERS, 3 * subs, nt, 128), BF16),
        pltpu.VMEM((ITERS, 3 * subs, nt, 128), BF16),
        pltpu.VMEM((subs, nt, 128), F32),
        pltpu.VMEM((ITERS, subs, nt, 128), BF16),
        pltpu.VMEM((ITERS, subs - 1, nt, 128), BF16),
        pltpu.VMEM((128, 128), F32),
        pltpu.VMEM((ITERS, 2, 1, 128), F32),
        pltpu.VMEM((ITERS, plan.cube, 1, 128), F32),
        pltpu.VMEM((plan.plane, chunk, 128), F32),
        pltpu.VMEM((plan.plane, chunk, 128), F32),
        pltpu.VMEM((plan.line, chunk, 128), F32),
        pltpu.VMEM((plan.plane, chunk, 128), F32),
        pltpu.SemaphoreType.DMA((6,)),
        pltpu.SemaphoreType.DMA((13,)),
        pltpu.SemaphoreType.DMA((13,)),
        pltpu.SemaphoreType.REGULAR,
    ]
    shapes = (
        jax.ShapeDtypeStruct((ITERS, local), F32),
        jax.ShapeDtypeStruct((j0 + ITERS, 2, k0 + ITERS), F32),
        jax.ShapeDtypeStruct((ITERS, j0 + ITERS), F32),
    )

    def pin(array):
        return pltpu.with_memory_space_constraint(array, pltpu.HBM)

    outs = pl.pallas_call(
        functools.partial(body, plan, k0, j0, unknowns, slots, nt),
        out_shape=shapes,
        in_specs=[hbm, hbm, hbm, hbm, smem, hbm, hbm],
        out_specs=(vmem, vmem, vmem),
        scratch_shapes=scratch,
        compiler_params=pltpu.CompilerParams(
            collective_id=0, has_side_effects=True, vmem_limit_bytes=48 << 20
        ),
        name="toar",
    )(
        pin(stiffness.reshape(stiffness.shape[2:])), pin(damping.reshape(damping.shape[2:])),
        pin(tile_map.reshape(2, slots)), pin(mass.reshape(nt, 128)), shift.reshape(1), pin(basis),
        pin(compact.transpose(2, 0, 1)),
    )
    new, comp, hess = pl.pallas_call(
        put_out,
        out_shape=shapes,
        in_specs=[vmem] * 3,
        out_specs=(hbm,) * 3,
        scratch_shapes=[pltpu.SemaphoreType.DMA((3,))],
        compiler_params=pltpu.CompilerParams(vmem_limit_bytes=2 << 20),
        name="put_out",
    )(*outs)
    return new, comp.transpose(1, 2, 0), hess.T


def solution(mesh):
    rows, subs = mesh.shape["rows"], mesh.shape["sub"]
    both = ("rows", "sub")
    return jax.shard_map(
        functools.partial(on_device, rows=rows, subs=subs),
        mesh=mesh,
        in_specs=(
            P("rows", "sub", None, None, None), P("rows", "sub", None, None, None),
            P("rows", "sub", None, None), P(both), P(), P(None, both), P(),
        ),
        out_specs=(P(None, both), P(), P()),
        check_vma=False,
    )
```

```python
import functools
import itertools

import jax
import jax.numpy as jnp
from jax import lax
from jax.experimental import pallas as pl
from jax.experimental.pallas import tpu as pltpu
from jax.sharding import PartitionSpec as P

ITERS = 2
EPS = 1e-06
MESH = pl.DeviceIdType.MESH
F32 = jnp.float32
BF16 = jnp.bfloat16
HELD = 60


def dot_nt(a, b):
    return lax.dot_general(a, b, (((1,), (1,)), ((), ())), preferred_element_type=F32)


def halves(x):
    hi = x.astype(BF16)
    return hi, (x - hi.astype(F32)).astype(BF16)


def iota(shape, dim):
    return lax.broadcasted_iota(jnp.int32, shape, dim)


def lane_sum(x):
    return jnp.sum(x, axis=1, keepdims=True)


def row_sum(x):
    return jnp.sum(x, axis=0, keepdims=True)


def tree_sum(terms):
    while len(terms) > 1:
        terms = [sum(terms[i + 1 : i + 2], terms[i]) for i in range(0, len(terms), 2)]
    return terms[0]


def ring_distance(step, size):
    return min(step, size - step)


class Plan:
    def __init__(self, rows, subs):
        self.rows, self.subs = rows, subs
        self.cores = 2
        self.ys = 4 if rows >= 32 else 2
        self.zs = rows // (self.ys * self.cores)
        self.plane = self.ys * subs
        self.line = self.zs * self.cores
        self.cube = self.zs * self.ys * subs

    def steps(self, *sizes):
        every = [s for s in itertools.product(*map(range, sizes)) if any(s)]
        return sorted(every, key=lambda s: -sum(map(ring_distance, s, sizes)))


def body(
    plan, k0, j0, unknowns, slots, nt,
    stiff_hbm, damp_hbm, map_hbm, mass_hbm, shift_ref, basis_hbm, compact_hbm,
    new_ref, comp_ref, hess_ref,
    tiles_d, tiles_k, nat, held, map_s, mass_s, compact_s, image_s, column_s, coef_u, coef_l,
    square_s, upper_m, lower_m, gram_m, split_s, onehot_g, onehot_s, window_l, window_u, part_f, part_s, part_r,
    parts_m, pair_r, cube_r, gram_s, gram_1, gram_2, gram_3,
    copy_sem, send_sem, recv_sem, ready_sem,
):
    rows, subs = plan.rows, plan.subs
    basis_copy = pltpu.make_async_copy(basis_hbm, nat, copy_sem.at[0])
    basis_copy.start()

    row = lax.axis_index("rows")
    sub = lax.axis_index("sub")
    core = lax.rem(row, plan.cores)
    chip = lax.div(row, plan.cores)
    y = lax.rem(chip, plan.ys)
    z = lax.div(chip, plan.ys)
    in_plane = y * subs + sub
    in_line = z * plan.cores + core
    in_cube = chip * subs + sub
    to_x = [lax.rem(sub + i, subs) for i in range(subs)]
    to_y = [lax.rem(y + i, plan.ys) for i in range(plan.ys)]
    to_z = [lax.rem(z + i, plan.zs) for i in range(plan.zs)]
    to_c = [core, 1 - core]
    above = lax.rem(row + rows - 1, rows)
    below = lax.rem(row + 1, rows)

    def at(dz, dy, dc, dx):
        return ((to_z[dz] * plan.ys + to_y[dy]) * plan.cores + to_c[dc], to_x[dx])

    plane_peers = [
        (to_y[dy] * subs + to_x[dx], at(0, dy, 0, dx)) for dy, dx in plan.steps(plan.ys, subs)
    ]
    line_peers = [at(dz, 0, dc, 0) for dz, dc in plan.steps(plan.zs, plan.cores)]
    partner = row + 1 - 2 * core
    across = jnp.where(core == 0, above, below)
    to_partner = jnp.where(core == 0, 0, 2 * subs)
    to_across = 2 * subs - to_partner
    far_first = sorted(range(subs), key=lambda i: -ring_distance(i, subs))

    barrier = pltpu.get_barrier_semaphore()
    greeted = line_peers + [(across, x) for x in to_x] + [device for _, device in plane_peers]
    for device in greeted:
        pl.semaphore_signal(barrier, inc=1, device_id=device, device_id_type=MESH)

    small = [
        pltpu.make_async_copy(compact_hbm, compact_s, copy_sem.at[1]),
        pltpu.make_async_copy(map_hbm, map_s, copy_sem.at[2]),
        pltpu.make_async_copy(mass_hbm, mass_s, copy_sem.at[3]),
    ]
    for copy in small:
        copy.start()

    def send(src, dst, which, device):
        pltpu.make_async_remote_copy(
            src_ref=src, dst_ref=dst, send_sem=send_sem.at[which], recv_sem=recv_sem.at[which],
            device_id=device, device_id_type=MESH,
        ).start()

    def arrived(view, which):
        pltpu.make_async_copy(view, view, recv_sem.at[which]).wait()

    def departed(view, which):
        pltpu.make_async_copy(view, view, send_sem.at[which]).wait()

    shift = shift_ref[0]
    scale = 1.0 / unknowns
    eye64 = (iota((64, 128), 0) == iota((64, 128), 1)).astype(F32)
    lane = iota((1, 128), 1)
    lane64 = iota((64, 128), 1)
    row64 = iota((64, 128), 0)
    held[k0 * nt :, :] = jnp.zeros((held.shape[0] - k0 * nt, 128), F32)

    small[0].wait()
    last = compact_s[j0 - 1]
    last = jnp.concatenate([last, jnp.zeros((2, 128 - k0), F32)], axis=1)
    u1 = jnp.broadcast_to(lane_sum(eye64 * last[0:1]), (64, 128))
    u2 = jnp.broadcast_to(lane_sum(eye64 * last[1:2]), (64, 128))
    coef_u[...] = u1
    coef_l[...] = u2

    basis_copy.wait()
    tile_copies = [
        pltpu.make_async_copy(damp_hbm, tiles_d, copy_sem.at[4]),
        pltpu.make_async_copy(stiff_hbm, tiles_k, copy_sem.at[5]),
    ]
    for copy in tile_copies:
        copy.start()

    def regroup(b, carry):
        for i in range(4):
            t = b * 4 + i
            held[pl.ds(t, k0, stride=nt), :] = nat[:, pl.ds(pl.multiple_of(t * 128, 128), 128)]
        return carry

    lax.fori_loop(0, nt // 4, regroup, 0)

    def combined(ref):
        def add(b, total):
            for i in range(12):
                k = b * 12 + i
                h = held[pl.ds(pl.multiple_of(k * nt, 8), nt), :]
                total = total + h * jnp.broadcast_to(ref[pl.ds(k, 1), :], h.shape)
            return total
        return lax.fori_loop(0, HELD // 12, add, jnp.zeros((nt, 128), F32))

    def exchange(window, it, which, vector):
        mine = window.at[it, subs + sub]
        mine[...] = vector.astype(BF16)
        for step in far_first[:-1]:
            send(mine, mine, which, (row, to_x[step]))
        for step in far_first:
            send(mine, window.at[it, to_across + sub], which + 4, (across, to_x[step]))
        send(mine, window.at[it, to_partner + sub], which + 4, (partner, sub))

    def relay(window, it, which):
        arrived(window.at[it, pl.ds(0, subs - 1)], which)
        for step in far_first[:-1]:
            theirs = window.at[it, subs + to_x[step]]
            send(theirs, window.at[it, to_partner + to_x[step]], which + 4, (partner, sub))

    lower = combined(coef_l)
    pl.semaphore_wait(barrier, len(greeted))
    exchange(window_l, 0, 0, lower)
    upper = combined(coef_u)
    exchange(window_u, 0, 1, upper)
    for _, device in plane_peers:
        pl.semaphore_signal(ready_sem, inc=1, device_id=device, device_id_type=MESH)

    wide = nat.shape[1] // 8

    def gram_part(c, total):
        piece = nat[:, pl.ds(pl.multiple_of(c * wide, 128), wide)]
        hi, lo = halves(piece)
        split_s[0:k0, :] = hi
        split_s[64 : 64 + k0, :] = lo
        return total + dot_nt(split_s[...], split_s[0:64, :])

    def gram_ready():
        both = lax.fori_loop(0, 8, gram_part, jnp.zeros((128, 64), F32))
        cross = both[64:128]
        gram = both[0:64] + cross + cross.T
        gram = jnp.concatenate([gram, jnp.zeros((64, 64), F32)], axis=1)
        chunk = 64 // plan.plane
        for p in range(plan.plane):
            gram_s[p] = gram[p * chunk : (p + 1) * chunk]
        gram_1[in_plane] = gram_s[in_plane]

    column_s[...] = jnp.zeros_like(column_s)
    parts_m[...] = jnp.zeros_like(parts_m)
    split_s[...] = jnp.zeros_like(split_s)
    gram_ready()
    for peer, device in plane_peers:
        send(gram_s.at[peer], gram_1.at[in_plane], 14, device)

    for matrix, which in ((upper_m, 0), (lower_m, 1)):
        square_s[...] = jnp.zeros_like(square_s)
        square_s[0:j0, 0:k0] = compact_s[:, which, :]
        matrix[...] = square_s[...].T[0:64]
    comp_ref[...] = jnp.zeros_like(comp_ref)
    comp_ref[0:j0, :, 0:k0] = compact_s[...]

    small[1].wait()
    small[2].wait()
    target = map_s[0:1, :].astype(F32)
    source = map_s[1:2, :].astype(F32)
    onehot_s[...] = (
        jnp.broadcast_to(target, onehot_s.shape) == iota(onehot_s.shape, 0).astype(F32)
    ).astype(F32).astype(BF16)
    eye_s = (iota((slots, slots), 0) == iota((slots, slots), 1)).astype(F32)
    source_col = lane_sum(jnp.broadcast_to(source, (slots, slots)) * eye_s)
    spot = iota(onehot_g.shape, 1)
    first_tile = jnp.where(row == 0, subs * nt, 0)
    last_tile = jnp.where(row == rows - 1, 2 * subs * nt, 3 * subs * nt)
    hit = (
        (jnp.broadcast_to(source_col, onehot_g.shape) == spot.astype(F32))
        & (spot >= first_tile) & (spot < last_tile)
    )
    onehot_g[...] = hit.astype(F32).astype(BF16)

    mass = mass_s[...]
    block = min(64, slots)
    pair_s = lax.div(iota((128, slots), 1), 2)
    even_s = lax.rem(iota((slots, 128), 0), 2) == 0
    others = pl.ds(0, 2 * subs)
    peers = pl.ds(0, subs - 1)
    plane_view = pl.ds(0, plan.plane - 1)
    line_view = pl.ds(0, plan.line - 1)
    cube_view = pl.ds(0, plan.cube - 1)

    for it in range(ITERS):
        m, cols = k0 + it, j0 + it
        def products(tiles, window, which):
            arrived(window.at[it, others], which + 4)
            source = window[it].reshape(3 * subs * nt, 128)
            picked = jnp.dot(onehot_g[...], source, preferred_element_type=F32)
            even = jnp.where(even_s, picked, 0.0)
            picked = jnp.concatenate([even, picked - even], axis=1).astype(BF16)

            def some(b, total):
                t = tiles[pl.ds(b * block, block)].reshape(block // 2, 2, 128, 128)
                pairs = jnp.concatenate([t[:, 0], t[:, 1]], axis=2).reshape(block * 64, 256)
                r = dot_nt(pairs, picked)
                for i in range(block // 2):
                    here = pair_s == b * (block // 2) + i
                    total = jnp.where(here, r[i * 128 : (i + 1) * 128], total)
                return total

            return lax.fori_loop(0, slots // block, some, jnp.zeros((128, slots), F32))

        relay(window_l, it, 2 * it)
        relay(window_u, it, 2 * it + 1)
        if it == 0:
            for copy in tile_copies:
                copy.wait()
        product = products(tiles_k, window_l, 2 * it)
        product = product + products(tiles_d, window_u, 2 * it + 1)
        hi, lo = halves(product)
        part = dot_nt(onehot_s[...], hi) + dot_nt(onehot_s[...], lo)
        part_f[...] = part.reshape(subs, nt, 128)
        part_s[it] = part.reshape(subs, nt, 128).astype(BF16)
        for step in sorted(range(1, subs), key=lambda i: -ring_distance(i, subs)):
            send(part_s.at[it, to_x[step]], part_r.at[it, step - 1], 8 + it, (row, to_x[step]))
        if it == 0:
            arrived(gram_1.at[plane_view], 14)
            gram_2[in_line] = jnp.sum(gram_1[...], axis=0)
            for device in line_peers:
                send(gram_2.at[in_line], gram_2.at[in_line], 15, device)
        for which, window in ((2 * it, window_l), (2 * it + 1, window_u)):
            departed(window.at[it, peers], which)
            departed(window.at[it, others], which + 4)
        own = part_f[sub]
        arrived(part_r.at[it], 8 + it)
        coupled = own
        for step in range(1, subs):
            coupled = coupled + part_r[it, step - 1].astype(F32)
        image = shift * upper - mass * coupled
        image_s[...] = image

        def inner(b, total):
            for i in range(8):
                t = b * 8 + i
                piece = nat[:, pl.ds(pl.multiple_of(t * 128, 128), 128)]
                total = total + piece * jnp.broadcast_to(image_s[pl.ds(t, 1), :], piece.shape)
            return total

        parts_m[0:k0, :] = lax.fori_loop(0, nt // 8, inner, jnp.zeros((k0, 128), F32))
        if it > 0:
            parts_m[k0 : k0 + 1, :] = row_sum(column_s[...] * image)
        parts_m[63:64, :] = row_sum(image * image)
        pair_r[it, core] = row_sum(parts_m[...].T)
        send(pair_r.at[it, core], pair_r.at[it, core], 10 + it, at(0, 0, 1, 0))
        if it == 0:
            arrived(gram_2.at[line_view], 15)
            gram_3[in_plane] = jnp.sum(gram_2[...], axis=0)
            pl.semaphore_wait(ready_sem, plan.plane - 1)
        arrived(pair_r.at[it, 0], 10 + it)
        cube_r[it, in_cube] = pair_r[it, 0] + pair_r[it, 1]
        mine = cube_r.at[it, in_cube]
        for dz, dy, dx in plan.steps(plan.zs, plan.ys, subs):
            send(mine, mine, 12 + it, at(dz, dy, 0, dx))
        if it == 0:
            for _, device in plane_peers:
                send(gram_3.at[in_plane], gram_3.at[in_plane], 16, device)
        departed(part_r.at[it], 8 + it)
        departed(pair_r.at[it, 0], 10 + it)
        if it == 0:
            departed(gram_1.at[plane_view], 14)
            departed(gram_2.at[line_view], 15)
            departed(gram_3.at[plane_view], 16)
            arrived(gram_3.at[plane_view], 16)
            gram_m[...] = gram_3[...].reshape(64, 128) * scale
        gram = gram_m[...]
        turn = 2.0 * eye64 - gram
        up, low = upper_m[...], lower_m[...]
        lower_c = u1 + shift * u2
        arrived(cube_r.at[it, cube_view], 12 + it)
        sums = tree_sum([cube_r[it, i] for i in range(plan.cube)]) * scale

        own_square = lane_sum(jnp.where(lane == 63, sums, 0.0))
        first = jnp.where(lane < m, sums, 0.0)
        coef = jnp.broadcast_to(lane_sum(turn * first), (64, 128))
        coef_row = row_sum(eye64 * coef)
        gram_coef = row_sum(gram * coef)
        square = own_square + lane_sum(coef_row * (gram_coef - 2.0 * first))
        norm = jnp.sqrt(square + EPS)

        upper_c = jnp.where(row64 == m, norm, coef)
        weights = jnp.zeros((1, 128), F32)
        for _ in range(2):
            projection = row_sum(up * upper_c + low * lower_c)
            upper_c = upper_c - lane_sum(up * projection)
            lower_c = lower_c - lane_sum(low * projection)
            weights = weights + projection
        beta = jnp.sqrt(row_sum(upper_c * upper_c) + row_sum(lower_c * lower_c) + EPS)
        u1, u2 = upper_c / beta, lower_c / beta

        if it + 1 < ITERS:
            ratio = row_sum(jnp.where(row64 == m, u1, 0.0)) / norm
            coef_u[...] = u1 - ratio * coef
            coef_l[...] = u2
            exchange(window_l, it + 1, 2 * it + 2, combined(coef_l))
            upper = combined(coef_u) + ratio * image
            exchange(window_u, it + 1, 2 * it + 3, upper)
            upper_m[...] = jnp.where(lane64 == cols, u1, up)
            lower_m[...] = jnp.where(lane64 == cols, u2, low)
        coef_u[...] = coef
        column = (image - combined(coef_u)) / norm
        column_s[...] = column
        for t in range(nt):
            new_ref[it : it + 1, t * 128 : (t + 1) * 128] = column_s[t : t + 1, :]
        hess_ref[it : it + 1, :] = jnp.where(lane == cols, beta, weights)[:, 0 : j0 + ITERS]
        comp_ref[cols, 0:1, :] = row_sum(eye64 * u1)[:, 0 : k0 + ITERS]
        comp_ref[cols, 1:2, :] = row_sum(eye64 * u2)[:, 0 : k0 + ITERS]
        departed(cube_r.at[it, cube_view], 12 + it)
        if it + 1 < ITERS:
            held[m * nt : (m + 1) * nt, :] = column
            cross_row = (first - gram_coef) / norm
            cross_col = lane_sum(eye64 * cross_row)
            gram = jnp.where(row64 == m, cross_row, gram)
            gram = jnp.where(lane64 == m, cross_col, gram)
            gram = jnp.where((row64 == m) & (lane64 == m), square / (norm * norm), gram)
            gram_m[...] = gram


def put_out(*refs):
    ins, outs, sems = refs[:3], refs[3:6], refs[6]
    copies = [pltpu.make_async_copy(a, b, sems.at[i]) for i, (a, b) in enumerate(zip(ins, outs))]
    for copy in copies:
        copy.start()
    for copy in copies:
        copy.wait()


def on_device(stiffness, damping, tile_map, mass, shift, basis, compact, *, rows, subs):
    plan = Plan(rows, subs)
    k0, local = basis.shape
    j0 = compact.shape[2]
    slots = stiffness.shape[2]
    nt = local // 128
    unknowns = local * rows * subs
    chunk = 64 // plan.plane
    vmem = pl.BlockSpec(memory_space=pltpu.VMEM)
    hbm = pl.BlockSpec(memory_space=pltpu.HBM)
    smem = pl.BlockSpec(memory_space=pltpu.SMEM)
    scratch = [
        pltpu.VMEM((slots, 128, 128), BF16),
        pltpu.VMEM((slots, 128, 128), BF16),
        pltpu.VMEM((k0, local), F32),
        pltpu.VMEM((HELD * nt, 128), F32),
        pltpu.VMEM((2, slots), jnp.int32),
        pltpu.VMEM((nt, 128), F32),
        pltpu.VMEM((j0, 2, k0), F32),
        pltpu.VMEM((nt, 128), F32),
        pltpu.VMEM((nt, 128), F32),
        pltpu.VMEM((64, 128), F32),
        pltpu.VMEM((64, 128), F32),
        pltpu.VMEM((128, 128), F32),
        pltpu.VMEM((64, 128), F32),
        pltpu.VMEM((64, 128), F32),
        pltpu.VMEM((64, 128), F32),
        pltpu.VMEM((128, local // 8), BF16),
        pltpu.VMEM((slots, 3 * subs * nt), BF16),
        pltpu.VMEM((subs * nt, slots), BF16),
        pltpu.VMEM((ITERS, 3 * subs, nt, 128), BF16),
        pltpu.VMEM((ITERS, 3 * subs, nt, 128), BF16),
        pltpu.VMEM((subs, nt, 128), F32),
        pltpu.VMEM((ITERS, subs, nt, 128), BF16),
        pltpu.VMEM((ITERS, subs - 1, nt, 128), BF16),
        pltpu.VMEM((128, 128), F32),
        pltpu.VMEM((ITERS, 2, 1, 128), F32),
        pltpu.VMEM((ITERS, plan.cube, 1, 128), F32),
        pltpu.VMEM((plan.plane, chunk, 128), F32),
        pltpu.VMEM((plan.plane, chunk, 128), F32),
        pltpu.VMEM((plan.line, chunk, 128), F32),
        pltpu.VMEM((plan.plane, chunk, 128), F32),
        pltpu.SemaphoreType.DMA((6,)),
        pltpu.SemaphoreType.DMA((17,)),
        pltpu.SemaphoreType.DMA((17,)),
        pltpu.SemaphoreType.REGULAR,
    ]
    shapes = (
        jax.ShapeDtypeStruct((ITERS, local), F32),
        jax.ShapeDtypeStruct((j0 + ITERS, 2, k0 + ITERS), F32),
        jax.ShapeDtypeStruct((ITERS, j0 + ITERS), F32),
    )

    def pin(array):
        return pltpu.with_memory_space_constraint(array, pltpu.HBM)

    outs = pl.pallas_call(
        functools.partial(body, plan, k0, j0, unknowns, slots, nt),
        out_shape=shapes,
        in_specs=[hbm, hbm, hbm, hbm, smem, hbm, hbm],
        out_specs=(vmem, vmem, vmem),
        scratch_shapes=scratch,
        compiler_params=pltpu.CompilerParams(
            collective_id=0, has_side_effects=True, vmem_limit_bytes=48 << 20
        ),
        name="toar",
    )(
        pin(stiffness.reshape(stiffness.shape[2:])), pin(damping.reshape(damping.shape[2:])),
        pin(tile_map.reshape(2, slots)), pin(mass.reshape(nt, 128)), shift.reshape(1), pin(basis),
        pin(compact.transpose(2, 0, 1)),
    )
    new, comp, hess = pl.pallas_call(
        put_out,
        out_shape=shapes,
        in_specs=[vmem] * 3,
        out_specs=(hbm,) * 3,
        scratch_shapes=[pltpu.SemaphoreType.DMA((3,))],
        compiler_params=pltpu.CompilerParams(vmem_limit_bytes=2 << 20),
        name="put_out",
    )(*outs)
    return new, comp.transpose(1, 2, 0), hess.T


def solution(mesh):
    rows, subs = mesh.shape["rows"], mesh.shape["sub"]
    both = ("rows", "sub")
    return jax.shard_map(
        functools.partial(on_device, rows=rows, subs=subs),
        mesh=mesh,
        in_specs=(
            P("rows", "sub", None, None, None), P("rows", "sub", None, None, None),
            P("rows", "sub", None, None), P(both), P(), P(None, both), P(),
        ),
        out_specs=(P(None, both), P(), P()),
        check_vma=False,
    )
```
